32 devices in a mesh: dp: 1 (over z), tp: 4 (over y), cp: 8 (over x, core).
Axes of the slice: x: 4, y: 4, z: 1, core: 2. Of those that a mesh axis runs over, the one named last changes fastest.
The devices are a block of a 4x4x8 slice.
Arguments:
- x_suffix: bfloat16 [8192, 4096], P(('dp', 'cp'))
- k_prefix: bfloat16 [8192, 8, 128], P(('dp', 'cp'), 'tp')
- v_prefix: bfloat16 [8192, 8, 128], P(('dp', 'cp'), 'tp')
- norm_attn: bfloat16 [4096], replicated
- w_query: bfloat16 [4096, 4096], P(None, 'tp')
- w_key: bfloat16 [4096, 1024], P(None, 'tp')
- w_value: bfloat16 [4096, 1024], P(None, 'tp')
- w_out: bfloat16 [4096, 4096], P('tp')
- norm_mlp: bfloat16 [4096], replicated
- w_gate: bfloat16 [4096, 14336], P(None, 'tp')
- w_up: bfloat16 [4096, 14336], P(None, 'tp')
- w_down: bfloat16 [14336, 4096], P('tp')
Outputs:
- output 1: bfloat16 [8192, 4096], P(('dp', 'cp'))
- output 2: bfloat16 [8192, 8, 128], P(('dp', 'cp'), 'tp')
- output 3: bfloat16 [8192, 8, 128], P(('dp', 'cp'), 'tp')
All inputs are finite; a program needn't handle non-finite values.
Results may differ from the reference program's by a relative error of at most 0.0110871.
Values are sent between devices in bfloat16 or wider.
A program may use at most 768 MiB of HBM per device.

```python
import jax
import jax.numpy as jnp
from jax import lax

D = 4096
HEADS = 32
KV_HEADS = 8
HEAD = 128
FF = 14336
SEQ_GROUPS = 8
PREFIX_DEV = 1024
SUFFIX_BLK = 512

PREFIX = SEQ_GROUPS * PREFIX_DEV
SUFFIX = 2 * SEQ_GROUPS * SUFFIX_BLK
GROUP_RATIO = HEADS // KV_HEADS
ROPE_THETA = 500000.0
NORM_EPS = 1e-5


def setup_inputs(seed: int = 0, part: int = 0) -> dict:
    shared_keys = jax.random.split(jax.random.key(seed), 9)
    part_keys = jax.random.split(jax.random.fold_in(jax.random.key(seed + 1), part), 3)
    out_std = 2.0 * ((PREFIX + SUFFIX // 2) / (HEADS * HEAD)) ** 0.5

    def normal_draw(rng_key, dims, std_dev):
        return (jax.random.normal(rng_key, dims, jnp.float32) * std_dev).astype(jnp.bfloat16)

    def gain_draw(rng_key):
        return jax.random.uniform(rng_key, (D,), jnp.float32, 0.5, 1.5).astype(jnp.bfloat16)

    return {
        'x_suffix': normal_draw(part_keys[0], (SUFFIX, D), 1.0),
        'k_prefix': normal_draw(part_keys[1], (PREFIX, KV_HEADS, HEAD), 1.0),
        'v_prefix': normal_draw(part_keys[2], (PREFIX, KV_HEADS, HEAD), 1.0),
        'norm_attn': gain_draw(shared_keys[0]),
        'w_query': normal_draw(shared_keys[1], (D, HEADS * HEAD), D ** -0.5),
        'w_key': normal_draw(shared_keys[2], (D, KV_HEADS * HEAD), D ** -0.5),
        'w_value': normal_draw(shared_keys[3], (D, KV_HEADS * HEAD), D ** -0.5),
        'w_out': normal_draw(shared_keys[4], (HEADS * HEAD, D), out_std),
        'norm_mlp': gain_draw(shared_keys[5]),
        'w_gate': normal_draw(shared_keys[6], (D, FF), D ** -0.5),
        'w_up': normal_draw(shared_keys[7], (D, FF), D ** -0.5),
        'w_down': normal_draw(shared_keys[8], (FF, D), 2.0 * FF ** -0.5),
    }


def suffix_positions():
    row_ids = jnp.arange(SUFFIX, dtype=jnp.int32)
    owner_dev = row_ids // (2 * SUFFIX_BLK)
    local_row = row_ids % (2 * SUFFIX_BLK)
    blk_idx = jnp.where(local_row < SUFFIX_BLK, owner_dev, 2 * SEQ_GROUPS - 1 - owner_dev)
    return PREFIX + blk_idx * SUFFIX_BLK + local_row % SUFFIX_BLK


def rope_tables(positions):
    inv_freq = ROPE_THETA ** (-jnp.arange(0, HEAD, 2, dtype=jnp.float32) / HEAD)
    angles = positions.astype(jnp.float32)[:, None] * inv_freq[None, :]
    return jnp.cos(angles), jnp.sin(angles)


def apply_rope(values, cos_tab, sin_tab):
    half_dim = HEAD // 2
    first_half = values[..., :half_dim]
    second_half = values[..., half_dim:]
    cos_rows = cos_tab[:, None, :]
    sin_rows = sin_tab[:, None, :]
    return jnp.concatenate([first_half * cos_rows - second_half * sin_rows, second_half * cos_rows + first_half * sin_rows], axis=-1)


def rms_norm(values, gain_vec):
    vals32 = values.astype(jnp.float32)
    inv_rms = lax.rsqrt(jnp.mean(vals32 * vals32, axis=-1, keepdims=True) + NORM_EPS)
    return (vals32 * inv_rms * gain_vec.astype(jnp.float32)).astype(jnp.bfloat16)


def reference(x_suffix, k_prefix, v_prefix, norm_attn, w_query, w_key, w_value, w_out, norm_mlp, w_gate, w_up, w_down):
    positions = suffix_positions()
    cos_tab, sin_tab = rope_tables(positions)
    hidden = rms_norm(x_suffix, norm_attn)
    q_proj = jnp.dot(hidden, w_query, preferred_element_type=jnp.float32).reshape(SUFFIX, HEADS, HEAD)
    q_rot = apply_rope(q_proj, cos_tab, sin_tab).astype(jnp.bfloat16)
    k_proj = jnp.dot(hidden, w_key, preferred_element_type=jnp.float32).reshape(SUFFIX, KV_HEADS, HEAD)
    k_suffix = apply_rope(k_proj, cos_tab, sin_tab).astype(jnp.bfloat16)
    v_suffix = jnp.dot(hidden, w_value, preferred_element_type=jnp.float32).astype(jnp.bfloat16).reshape(SUFFIX, KV_HEADS, HEAD)
    keys_all = jnp.moveaxis(jnp.concatenate([k_prefix, k_suffix], axis=0), 1, 0)
    vals_all = jnp.moveaxis(jnp.concatenate([v_prefix, v_suffix], axis=0), 1, 0)
    key_pos = jnp.concatenate([jnp.arange(PREFIX, dtype=jnp.int32), positions])
    q_blocks = jnp.moveaxis(q_rot.reshape(2 * SEQ_GROUPS, SUFFIX_BLK, KV_HEADS, GROUP_RATIO, HEAD), 2, 1)
    pos_blocks = positions.reshape(2 * SEQ_GROUPS, SUFFIX_BLK)
    score_scale = HEAD ** -0.5

    def attend_block(blk_args):
        q_blk, q_pos = blk_args
        visible = (key_pos[None, :] <= q_pos[:, None])[:, None, :]

        def attend_head(head_args):
            q_head, k_head, v_head = head_args
            scores = jnp.einsum('brd,kd->brk', q_head.astype(jnp.float32), k_head.astype(jnp.float32)) * score_scale
            scores = jnp.where(visible, scores, -jnp.inf)
            row_max = jnp.max(scores, axis=-1, keepdims=True)
            weights = jnp.exp(scores - row_max)
            denom_sum = jnp.sum(weights, axis=-1, keepdims=True)
            numer_sum = jnp.einsum('brk,kd->brd', weights.astype(jnp.bfloat16).astype(jnp.float32), v_head.astype(jnp.float32))
            return (numer_sum / denom_sum).astype(jnp.bfloat16)

        return lax.map(attend_head, (q_blk, keys_all, vals_all))

    attn_heads = lax.map(attend_block, (q_blocks, pos_blocks))
    attn_heads = jnp.moveaxis(attn_heads, 1, 2).reshape(SUFFIX, HEADS * HEAD)
    resid_mid = x_suffix.astype(jnp.float32) + jnp.dot(attn_heads, w_out, preferred_element_type=jnp.float32)
    hidden_mlp = rms_norm(resid_mid, norm_mlp)
    gate_proj = jnp.dot(hidden_mlp, w_gate, preferred_element_type=jnp.float32)
    up_proj = jnp.dot(hidden_mlp, w_up, preferred_element_type=jnp.float32)
    act_mid = (jax.nn.silu(gate_proj) * up_proj).astype(jnp.bfloat16)
    x_out = (resid_mid + jnp.dot(act_mid, w_down, preferred_element_type=jnp.float32)).astype(jnp.bfloat16)
    return (x_out, k_suffix, v_suffix)
```

```python
import functools

import jax
import jax.numpy as jnp
from jax import lax
from jax.experimental import pallas as pl
from jax.experimental.pallas import tpu as pltpu
from jax.sharding import PartitionSpec as P

ROPE_THETA = 500000.0
NORM_EPS = 1e-5
LOG2E = 1.4426950408889634
KEY_BLOCK = 512


def rope_tables(positions, head_dim):
    inv_freq = ROPE_THETA ** (-jnp.arange(0, head_dim, 2, dtype=jnp.float32) / head_dim)
    angles = positions.astype(jnp.float32)[:, None] * inv_freq[None, :]
    return jnp.cos(angles), jnp.sin(angles)


def apply_rope(values, cos_tab, sin_tab):
    half_dim = values.shape[-1] // 2
    first_half = values[..., :half_dim]
    second_half = values[..., half_dim:]
    cos_rows = cos_tab[:, None, :]
    sin_rows = sin_tab[:, None, :]
    return jnp.concatenate([first_half * cos_rows - second_half * sin_rows, second_half * cos_rows + first_half * sin_rows], axis=-1)


def rms_norm(values, gain_vec):
    vals32 = values.astype(jnp.float32)
    inv_rms = lax.rsqrt(jnp.mean(vals32 * vals32, axis=-1, keepdims=True) + NORM_EPS)
    return (vals32 * inv_rms * gain_vec.astype(jnp.float32)).astype(jnp.bfloat16)


def flash_kernel(groups, key_rows, use_prefix, use_suffix, second_block, q_row0, has_state, *refs):
    refs = list(refs)
    q_ref = refs.pop(0)
    state_ref = refs.pop(0) if has_state else None
    n_parts = int(use_prefix) + int(use_suffix)
    n_slots = groups * n_parts
    per_part = groups + 2
    src_refs = [refs.pop(0) for _ in range(per_part * n_parts)]
    out_ref = refs.pop(0)
    kv_scr, s_scr, sems = refs
    head_dim = q_ref.shape[-1]
    tq = q_ref.shape[0]
    scale = (head_dim ** -0.5) * LOG2E
    group = pl.program_id(0)
    n_groups = kv_scr.shape[0]

    def copies(g):
        out = []
        for part in range(n_parts):
            for slot in range(groups):
                if slot < groups - 2:
                    src = src_refs[part * per_part + slot].at[g]
                else:
                    src = src_refs[part * per_part + groups - 2 + (slot - groups + 2) * 2 + g]
                dst_slot = part * groups + slot
                out.append(pltpu.make_async_copy(src, kv_scr.at[g, dst_slot], sems.at[g, dst_slot]))
        return out

    first = (pl.program_id(1) == 0) & (pl.program_id(2) == 0)

    @pl.when(first & (group == 0))
    def _():
        for g in range(n_groups):
            for cp in copies(g):
                cp.start()
        for cp in copies(0):
            cp.wait()

    for g in range(1, n_groups):
        @pl.when(first & (group == g))
        def _():
            for cp in copies(g):
                cp.wait()

    me = lax.axis_index('cp')
    my_x, my_core = me // 2, me % 2
    blk = (2 * groups - 1 - me) if second_block else me
    half = key_rows // 2
    q = q_ref[...]

    def locate(j):
        n_pre = 2 * groups if use_prefix else 0
        b = j - n_pre
        lower = b < groups
        dev = jnp.where(lower, b, 2 * groups - 1 - b)
        rel = (dev // 2 - my_x + groups // 2) % (groups // 2)
        order = jnp.where(rel == 0, 0, jnp.where(rel == 1, 2, jnp.where(rel == 2, 3, 1)))
        s_slot = order * 2 + jnp.where(dev % 2 == my_core, 0, 1) + (groups if use_prefix else 0)
        s_off = jnp.where(lower, 0, half)
        if not use_suffix:
            return j // 2, (j % 2) * half
        if not use_prefix:
            return s_slot, s_off
        pre = j < n_pre
        return jnp.where(pre, j // 2, s_slot), jnp.where(pre, (j % 2) * half, s_off)

    def scores(j):
        slot, off = locate(j)
        k = kv_scr[group, slot, pl.ds(pl.multiple_of(off, half), half), :]
        return lax.dot_general(k, q, (((1,), (1,)), ((), ())), preferred_element_type=jnp.float32)

    def values_t(j):
        slot, off = locate(j)
        v = kv_scr[group, slot, pl.ds(pl.multiple_of(key_rows + off, half), half), :]
        return jnp.concatenate([v[i * head_dim:(i + 1) * head_dim] for i in range(half // head_dim)], axis=1)

    def update(s, v, state):
        m, l, acc = state
        n = s.shape[0]
        folded = jnp.max(s.reshape(n // 8, 8, tq), axis=0)
        m_new = jnp.maximum(m, jnp.max(folded, axis=0, keepdims=True))
        a = jnp.exp2((m - m_new) * scale)
        p = jnp.exp2(s * scale - m_new * scale)
        l = l * a + jnp.sum(p.reshape(n // 8, 8, tq), axis=0)
        acc = acc * a + jnp.dot(v, p.astype(jnp.bfloat16), preferred_element_type=jnp.float32)
        return m_new, l, acc

    n_pre = 2 * groups if use_prefix else 0
    n_full = n_pre + (blk if use_suffix else 0)
    last = n_full if use_suffix else n_full - 1
    if has_state:
        st = state_ref[0]
        state = (st[head_dim + 8:head_dim + 9], st[head_dim:head_dim + 8], st[:head_dim])
    else:
        state = (jnp.full((1, tq), -jnp.inf, jnp.float32), jnp.zeros((8, tq), jnp.float32), jnp.zeros((head_dim, tq), jnp.float32))

    s_scr[0] = scores(0)

    def make_body(base, unroll):
        def body(i, st):
            for u in range(unroll):
                j = base + i * unroll + u
                s_scr[(u + 1) % 2] = scores(jnp.minimum(j + 1, last))
                st = update(s_scr[u % 2], values_t(j), st)
            return st
        return body

    if use_prefix:
        state = lax.fori_loop(0, n_pre // 4, make_body(0, 4), state)
    if use_suffix:
        state = lax.fori_loop(0, blk // 2, make_body(n_pre, 2), state)

        def odd_body(i, st):
            s_scr[1] = scores(last)
            return update(s_scr[0], values_t(last - 1), st)

        state = lax.fori_loop(0, blk % 2, odd_body, state)
        s = s_scr[blk % 2]
        kid = lax.broadcasted_iota(jnp.int32, s.shape, 0)
        qid = lax.broadcasted_iota(jnp.int32, s.shape, 1) + (q_row0 + pl.program_id(2) * tq) % half
        state = update(jnp.where(kid <= qid, s, -jnp.inf), values_t(last), state)
        m, l, acc = state
        out = acc / jnp.sum(l, axis=0, keepdims=True)
        out_ref[...] = out.T.astype(out_ref.dtype)
    else:
        m, l, acc = state
        out_ref[0, :head_dim] = acc
        out_ref[0, head_dim:head_dim + 8] = l
        out_ref[0, head_dim + 8:] = jnp.broadcast_to(m, (8, tq))


def flash(q, kv_parts, groups, kv_heads, head_dim, second_block, row0, rows, use_prefix, use_suffix, state=None, tq=512):
    heads = q.shape[1] // head_dim
    ratio = heads // kv_heads
    key_rows = kv_parts[0][0].shape[1] // 2
    tq = min(tq, rows)
    t0 = row0 // tq
    n_parts = len(kv_parts)
    q_spec = pl.BlockSpec((tq, head_dim), lambda g, r, t: (t0 + t, g * ratio + r))
    st_spec = pl.BlockSpec((1, head_dim + 16, tq), lambda g, r, t: (g * ratio + r, 0, t))
    flat = [a for part in kv_parts for a in part]
    args, specs = [q], [q_spec]
    if state is not None:
        args.append(state)
        specs.append(st_spec)
    args += flat
    specs += [pl.BlockSpec(memory_space=pl.ANY)] * len(flat)
    if use_suffix:
        out_shape = jax.ShapeDtypeStruct((rows, heads * head_dim), jnp.bfloat16)
        out_spec = pl.BlockSpec((tq, head_dim), lambda g, r, t: (t, g * ratio + r))
    else:
        out_shape = jax.ShapeDtypeStruct((heads, head_dim + 16, rows), jnp.float32)
        out_spec = st_spec
    n_keys = (2 * groups * use_prefix + (groups + groups // 2 if second_block else groups // 2) * use_suffix) * (key_rows // 2)
    return pl.pallas_call(
        functools.partial(flash_kernel, groups, key_rows, use_prefix, use_suffix, second_block, row0, state is not None),
        grid=(kv_heads, ratio, rows // tq),
        in_specs=specs,
        out_specs=out_spec,
        out_shape=out_shape,
        scratch_shapes=[
            pltpu.VMEM((kv_heads, groups * n_parts, 2 * key_rows, head_dim), jnp.bfloat16),
            pltpu.VMEM((2, key_rows // 2, tq), jnp.float32),
            pltpu.SemaphoreType.DMA((kv_heads, groups * n_parts)),
        ],
        compiler_params=pltpu.CompilerParams(vmem_limit_bytes=48 * 2**20, dimension_semantics=("arbitrary",) * 3),
        cost_estimate=pl.CostEstimate(flops=rows * heads * n_keys * 4 * head_dim, bytes_accessed=16 * 2**20, transcendentals=rows * heads * n_keys),
        name="flash",
    )(*args)


def solution(mesh):
    groups = mesh.shape['cp']
    tp = mesh.shape['tp']
    up = [(i, (i + 1) % tp) for i in range(tp)]
    down = [(i, (i - 1) % tp) for i in range(tp)]
    x_up = [(i, (i + 2) % groups) for i in range(groups)]
    x_down = [(i, (i - 2) % groups) for i in range(groups)]
    sibling = [(i, i ^ 1) for i in range(groups)]

    def ring_kv(bundle):
        r1 = lax.ppermute(bundle, 'cp', x_up)
        l1 = lax.ppermute(bundle, 'cp', x_down)
        own_s = lax.ppermute(bundle, 'cp', sibling)
        r2 = lax.ppermute(r1[0], 'cp', x_up)
        l2 = lax.ppermute(l1[1], 'cp', x_down)
        r1_s = lax.ppermute(r1, 'cp', sibling)
        l1_s = lax.ppermute(l1, 'cp', sibling)
        r2_s = lax.ppermute(r2, 'cp', sibling)
        l2_s = lax.ppermute(l2, 'cp', sibling)
        return [bundle, own_s, r1, r1_s, l1, l1_s, r2, l2, r2_s, l2_s]

    def tp_pieces(z):
        h = z.shape[0] // 2
        r1 = lax.ppermute(z, 'tp', up)
        l1 = lax.ppermute(z, 'tp', down)
        r2 = lax.ppermute(r1[:h], 'tp', up)
        l2 = lax.ppermute(l1[h:], 'tp', down)
        return r1, l1, r2, l2

    def local_layer(x_loc, kp_loc, vp_loc, norm_attn, w_query, w_key, w_value, w_out, norm_mlp, w_gate, w_up, w_down):
        rows_loc = x_loc.shape[0]
        blk_len = rows_loc // 2
        pre_dev, kv_loc, head_dim = kp_loc.shape
        heads_loc = w_query.shape[1] // head_dim
        prefix_len = pre_dev * groups
        my_cp = lax.axis_index('cp')
        my_tp = lax.axis_index('tp')

        def bundle_of(k, v):
            kt = jnp.moveaxis(k, 1, 0)
            vt = v.reshape(rows_loc // head_dim, head_dim, kv_loc, head_dim).transpose(2, 0, 3, 1).reshape(kv_loc, rows_loc, head_dim)
            return jnp.concatenate([kt, vt], axis=1)

        pre_slots = ring_kv(bundle_of(kp_loc, vp_loc))

        w_rows = w_out.shape[0] // groups
        w_out_full = lax.all_gather(lax.dynamic_slice_in_dim(w_out, my_cp * w_rows, w_rows, 0), ('tp', 'cp'), tiled=True)

        local_row = jnp.arange(rows_loc, dtype=jnp.int32)
        blk_idx = jnp.where(local_row < blk_len, my_cp, 2 * groups - 1 - my_cp)
        q_pos = prefix_len + blk_idx * blk_len + local_row % blk_len
        cos_tab, sin_tab = rope_tables(q_pos, head_dim)
        hidden = rms_norm(x_loc, norm_attn)
        k_proj = jnp.dot(hidden, w_key, preferred_element_type=jnp.float32).reshape(rows_loc, kv_loc, head_dim)
        k_new = apply_rope(k_proj, cos_tab, sin_tab).astype(jnp.bfloat16)
        v_new = jnp.dot(hidden, w_value, preferred_element_type=jnp.float32).astype(jnp.bfloat16).reshape(rows_loc, kv_loc, head_dim)
        suf_slots = ring_kv(bundle_of(k_new, v_new))
        q_proj = jnp.dot(hidden, w_query, preferred_element_type=jnp.float32).reshape(rows_loc, heads_loc, head_dim)
        q_rot = apply_rope(q_proj, cos_tab, sin_tab).astype(jnp.bfloat16).reshape(rows_loc, heads_loc * head_dim)

        fl = functools.partial(flash, groups=groups, kv_heads=kv_loc, head_dim=head_dim)
        st_a = fl(q_rot, [pre_slots], second_block=False, row0=0, rows=blk_len, use_prefix=True, use_suffix=False)
        o_a = fl(q_rot, [suf_slots], second_block=False, row0=0, rows=blk_len, use_prefix=False, use_suffix=True, state=st_a)
        q_b, o_a = lax.optimization_barrier((q_rot, o_a))
        o_b = fl(q_b, [pre_slots, suf_slots], second_block=True, row0=blk_len, rows=blk_len, use_prefix=True, use_suffix=True)

        def gather_heads(o):
            r1, l1, r2, l2 = tp_pieces(o)
            width = o.shape[1]
            far = jnp.concatenate([r2, l2], axis=0)
            full = jnp.zeros((o.shape[0], width * tp), o.dtype)
            for piece, off in ((o, 0), (r1, -1), (l1, 1), (far, 2)):
                full = lax.dynamic_update_slice(full, piece, (0, ((my_tp + off) % tp) * width))
            return full

        def mlp(x_rows, o_full):
            rows = x_rows.shape[0]
            shard = rows // tp
            h = shard // 2
            resid = x_rows.astype(jnp.float32) + jnp.dot(o_full, w_out_full, preferred_element_type=jnp.float32)
            hidden_mlp = rms_norm(resid, norm_mlp)
            gate_proj = jnp.dot(hidden_mlp, w_gate, preferred_element_type=jnp.float32)
            up_proj = jnp.dot(hidden_mlp, w_up, preferred_element_type=jnp.float32)
            act = (jax.nn.silu(gate_proj) * up_proj).astype(jnp.bfloat16)
            part = jnp.dot(act, w_down, preferred_element_type=jnp.float32)

            def rows_of(arr, off, lo, n):
                return lax.dynamic_slice_in_dim(arr, ((my_tp + off) % tp) * shard + lo, n, 0)

            far_r = lax.ppermute(rows_of(part, 2, 0, h), 'tp', up)
            far_l = lax.ppermute(rows_of(part, 2, h, h), 'tp', down)
            to_up = jnp.concatenate([rows_of(part, 1, 0, h) + far_r, rows_of(part, 1, h, h)], axis=0)
            to_down = jnp.concatenate([rows_of(part, -1, 0, h), rows_of(part, -1, h, h) + far_l], axis=0)
            from_down = lax.ppermute(to_up, 'tp', up)
            from_up = lax.ppermute(to_down, 'tp', down)
            mine = (rows_of(resid, 0, 0, shard) + (rows_of(part, 0, 0, shard) + from_down + from_up)).astype(jnp.bfloat16)
            r1, l1, r2, l2 = tp_pieces(mine)
            return [(mine, 0, 0), (r1, -1, 0), (l1, 1, 0), (r2, 2, 0), (l2, 2, h)], shard

        x_out = jnp.zeros(x_loc.shape, x_loc.dtype)
        for row0, o in ((0, o_a), (blk_len, o_b)):
            pieces, shard = mlp(x_loc[row0:row0 + o.shape[0]], gather_heads(o))
            for piece, off, lo in pieces:
                x_out = lax.dynamic_update_slice(x_out, piece, (row0 + ((my_tp + off) % tp) * shard + lo, 0))
        return x_out, k_new, v_new

    row_spec = P(('dp', 'cp'), None)
    kv_spec = P(('dp', 'cp'), 'tp', None)
    col_spec = P(None, 'tp')
    row_split = P('tp', None)
    vec_spec = P(None)
    return jax.shard_map(local_layer, mesh=mesh, in_specs=(row_spec, kv_spec, kv_spec, vec_spec, col_spec, col_spec, col_spec, row_split, vec_spec, col_spec, col_spec, row_split), out_specs=(row_spec, kv_spec, kv_spec), check_vma=False)
```

```python
import functools

import jax
import jax.numpy as jnp
from jax import lax
from jax.experimental import pallas as pl
from jax.experimental.pallas import tpu as pltpu
from jax.sharding import PartitionSpec as P

ROPE_THETA = 500000.0
NORM_EPS = 1e-5
LOG2E = 1.4426950408889634
KEY_BLOCK = 512


def rope_tables(positions, head_dim):
    inv_freq = ROPE_THETA ** (-jnp.arange(0, head_dim, 2, dtype=jnp.float32) / head_dim)
    angles = positions.astype(jnp.float32)[:, None] * inv_freq[None, :]
    return jnp.cos(angles), jnp.sin(angles)


def apply_rope(values, cos_tab, sin_tab):
    half_dim = values.shape[-1] // 2
    first_half = values[..., :half_dim]
    second_half = values[..., half_dim:]
    cos_rows = cos_tab[:, None, :]
    sin_rows = sin_tab[:, None, :]
    return jnp.concatenate([first_half * cos_rows - second_half * sin_rows, second_half * cos_rows + first_half * sin_rows], axis=-1)


def rms_norm(values, gain_vec):
    vals32 = values.astype(jnp.float32)
    inv_rms = lax.rsqrt(jnp.mean(vals32 * vals32, axis=-1, keepdims=True) + NORM_EPS)
    return (vals32 * inv_rms * gain_vec.astype(jnp.float32)).astype(jnp.bfloat16)


def attn_kernel(cfg, *refs):
    groups, tp, kv_heads, ratio, head_dim, key_rows, rows, ring, upper = (
        cfg[k] for k in ('groups', 'tp', 'kv_heads', 'ratio', 'head_dim', 'key_rows', 'rows', 'ring', 'upper'))
    heads = kv_heads * ratio
    if ring:
        q_ref, pre_ref, suf_ref, o_full, kv_out, kv_scr, s_scr, o_scr, st_scr, kv_send, kv_recv, kv_save, o_send, o_recv, o_local = refs
    else:
        q_ref, kv_in, o_full, kv_scr, s_scr, o_scr, kv_recv, o_send, o_recv, o_local = refs
    me, my_tp = lax.axis_index('cp'), lax.axis_index('tp')
    my_x, my_core = me // 2, me % 2
    half = key_rows // 2
    scale = (head_dim ** -0.5) * LOG2E
    MESH = pl.DeviceIdType.MESH
    sib = {'cp': my_x * 2 + (1 - my_core)}
    x_next = {'cp': (me + 2) % groups}
    x_prev = {'cp': (me + groups - 2) % groups}
    peers = [{'tp': (my_tp + k) % tp} for k in range(1, tp)]

    barrier = pltpu.get_barrier_semaphore()
    greet = peers + ([sib, x_next, x_prev] if ring else [])
    for dev in greet:
        pl.semaphore_signal(barrier, inc=1, device_id=dev, device_id_type=MESH)
    pl.semaphore_wait(barrier, len(greet))

    def kv_copy(part, g, slot):
        base = part * groups
        src_own = (pre_ref, suf_ref)[part].at[g] if ring else None
        dst = kv_scr.at[g, base + slot]
        if slot == 0:
            return pltpu.make_async_copy(src_own, dst, kv_recv.at[g, base])
        if slot in (1, 2, 3):
            src = src_own
        elif slot in (4, 5):
            src = kv_scr.at[g, base + slot - 2]
        elif slot == 6:
            src = kv_scr.at[g, base + (2 if g == 0 else 3)]
        else:
            src = kv_scr.at[g, base + 6]
        dev = {1: sib, 4: sib, 5: sib, 7: sib, 2: x_next, 3: x_prev, 6: x_next if g == 0 else x_prev}[slot]
        return pltpu.make_async_remote_copy(src_ref=src, dst_ref=dst, send_sem=kv_send.at[g, base + slot], recv_sem=kv_recv.at[g, base + slot], device_id=dev, device_id_type=MESH)

    gs = range(kv_heads)

    def start(part, slots):
        for slot in slots:
            for g in gs:
                kv_copy(part, g, slot).start()

    def arrived(part, slots):
        for slot in slots:
            for g in gs:
                copy = kv_copy(part, g, slot)
                copy.wait() if slot == 0 else copy.wait_recv()

    blk = (2 * groups - 1 - me) if upper else me
    n_pre = 2 * groups

    def locate(j):
        b = j - n_pre
        lower = b < groups
        dev = jnp.where(lower, b, 2 * groups - 1 - b)
        rel = (dev // 2 - my_x + groups // 2) % (groups // 2)
        same = dev % 2 == my_core
        s_slot = jnp.where(rel == 0, jnp.where(same, 0, 1), jnp.where(rel == 1, jnp.where(same, 3, 5), jnp.where(rel == 2, jnp.where(same, 6, 7), jnp.where(same, 2, 4))))
        pre = j < n_pre
        return jnp.where(pre, j // 2, groups + s_slot), jnp.where(pre, (j % 2) * half, jnp.where(lower, 0, half))

    def head_pass(h, lo, hi, suffix, load, store):
        g = h // ratio
        q = q_ref[:, pl.ds(pl.multiple_of(h * head_dim, head_dim), head_dim)]

        def scores(j):
            slot, off = locate(j)
            k = kv_scr[g, slot, pl.ds(pl.multiple_of(off, half), half), :]
            return lax.dot_general(k, q, (((1,), (1,)), ((), ())), preferred_element_type=jnp.float32)

        def values_t(j):
            slot, off = locate(j)
            v = kv_scr[g, slot, pl.ds(pl.multiple_of(key_rows + off, half), half), :]
            return jnp.concatenate([v[i * head_dim:(i + 1) * head_dim] for i in range(half // head_dim)], axis=1)

        def update(s, v, state):
            m, l, acc = state
            n = s.shape[0]
            folded = jnp.max(s.reshape(n // 8, 8, rows), axis=0)
            m_new = jnp.maximum(m, jnp.max(folded, axis=0, keepdims=True))
            a = jnp.exp2((m - m_new) * scale)
            p = jnp.exp2(s * scale - m_new * scale)
            l = l * a + jnp.sum(p.reshape(n // 8, 8, rows), axis=0)
            acc = acc * a + jnp.dot(v, p.astype(jnp.bfloat16), preferred_element_type=jnp.float32)
            return m_new, l, acc

        last = n_pre + blk if suffix else hi - 1
        if load:
            state = (st_scr[h, head_dim + 8:head_dim + 9], st_scr[h, head_dim:head_dim + 8], st_scr[h, :head_dim])
        else:
            state = (jnp.full((1, rows), -jnp.inf, jnp.float32), jnp.zeros((8, rows), jnp.float32), jnp.zeros((head_dim, rows), jnp.float32))
        s_scr[0] = scores(lo)

        def make_body(base, unroll):
            def body(i, st):
                for u in range(unroll):
                    j = base + i * unroll + u
                    s_scr[(u + 1) % 2] = scores(jnp.minimum(j + 1, last))
                    st = update(s_scr[u % 2], values_t(j), st)
                return st
            return body

        state = lax.fori_loop(0, (hi - lo) // 4, make_body(lo, 4), state)
        if suffix:
            state = lax.fori_loop(0, blk // 2, make_body(n_pre, 2), state)

            def odd_body(i, st):
                s_scr[1] = scores(last)
                return update(s_scr[0], values_t(last - 1), st)

            state = lax.fori_loop(0, blk % 2, odd_body, state)
            s = s_scr[blk % 2]
            kid = lax.broadcasted_iota(jnp.int32, s.shape, 0)
            qid = lax.broadcasted_iota(jnp.int32, s.shape, 1)
            state = update(jnp.where(kid <= qid, s, -jnp.inf), values_t(last), state)
        m, l, acc = state
        if store:
            st_scr[h, :head_dim] = acc
            st_scr[h, head_dim:head_dim + 8] = l
            st_scr[h, head_dim + 8:] = jnp.broadcast_to(m, (8, rows))
        else:
            o_scr[h] = (acc / jnp.sum(l, axis=0, keepdims=True)).T.astype(o_scr.dtype)

    def o_dst(h):
        return o_full.at[:, pl.ds(pl.multiple_of(my_tp * heads * head_dim + h * head_dim, head_dim), head_dim)]

    def o_copies(h):
        return [pltpu.make_async_remote_copy(src_ref=o_scr.at[h], dst_ref=o_dst(h), send_sem=o_send.at[k, h], recv_sem=o_recv.at[k, h], device_id=dev, device_id_type=MESH) for k, dev in enumerate(peers)]

    def o_own(h):
        return pltpu.make_async_copy(o_scr.at[h], o_dst(h), o_local.at[h])

    def loop_heads(lo_h, hi_h, lo, hi, suffix, load):
        def body(h, carry):
            head_pass(h, lo, hi, suffix, load, not suffix)
            if suffix:
                o_own(h).start()
                for copy in o_copies(h):
                    copy.start()
            return carry
        lax.fori_loop(lo_h, hi_h, body, 0)

    if ring:
        start(0, (0, 1, 2, 3))
        start(1, (0, 1, 2, 3))
        arrived(0, (0, 1))
        loop_heads(0, heads, 0, 4, False, False)
        arrived(0, (2, 3))
        start(0, (4, 5, 6))
        loop_heads(0, heads, 4, 8, False, True)
        arrived(0, (4, 5))
        loop_heads(0, heads, 8, 12, False, True)
        arrived(0, (6,))
        start(0, (7,))
        arrived(1, (0, 1, 2, 3))
        start(1, (4, 5, 6))
        arrived(0, (7,))
        arrived(1, (4, 5, 6))
        start(1, (7,))
        arrived(1, (7,))
        for g in gs:
            for s in range(2 * groups):
                pltpu.make_async_copy(kv_scr.at[g, s], kv_out.at[g, s], kv_save.at[g, s]).start()
        loop_heads(0, heads, 12, 16, True, True)
        for g in gs:
            for s in range(2 * groups):
                pltpu.make_async_copy(kv_scr.at[g, s], kv_out.at[g, s], kv_save.at[g, s]).wait()
            for part in range(2):
                for slot in range(1, groups):
                    kv_copy(part, g, slot).wait_send()
    else:
        def load_copy(g, s):
            return pltpu.make_async_copy(kv_in.at[g, s], kv_scr.at[g, s], kv_recv.at[g, s])
        for g in gs:
            for s in range(2 * groups):
                load_copy(g, s).start()
        for g in gs:
            for s in range(2 * groups):
                load_copy(g, s).wait()
            loop_heads(g * ratio, (g + 1) * ratio, 0, 16, True, False)

    def drain(h, carry):
        o_own(h).wait()
        for copy in o_copies(h):
            copy.wait()
        return carry

    lax.fori_loop(0, heads, drain, 0)


def attention(q, kv, cfg):
    groups, tp, kv_heads, ratio, head_dim, key_rows, rows, ring, upper = (
        cfg[k] for k in ('groups', 'tp', 'kv_heads', 'ratio', 'head_dim', 'key_rows', 'rows', 'ring', 'upper'))
    heads = kv_heads * ratio
    any_spec = pl.BlockSpec(memory_space=pl.ANY)
    row_blk = 1 if upper else 0
    q_spec = pl.BlockSpec((rows, heads * head_dim), lambda i: (row_blk, 0))
    o_shape = jax.ShapeDtypeStruct((rows, tp * heads * head_dim), jnp.bfloat16)
    kv_shape = (kv_heads, 2 * groups, 2 * key_rows, head_dim)
    scratch = [pltpu.VMEM(kv_shape, jnp.bfloat16), pltpu.VMEM((2, key_rows // 2, rows), jnp.float32), pltpu.VMEM((heads, rows, head_dim), jnp.bfloat16)]
    dma = pltpu.SemaphoreType.DMA
    kv_sem, o_sem = dma((kv_heads, 2 * groups)), dma((tp - 1, heads))
    if ring:
        out_shape, out_specs = (o_shape, jax.ShapeDtypeStruct(kv_shape, jnp.bfloat16)), (any_spec, any_spec)
        scratch += [pltpu.VMEM((heads, head_dim + 16, rows), jnp.float32), kv_sem, kv_sem, kv_sem, o_sem, o_sem, dma((heads,))]
    else:
        out_shape, out_specs = o_shape, any_spec
        scratch += [kv_sem, o_sem, o_sem, dma((heads,))]
    n_keys = (2 * groups + (groups + groups // 2 if upper else groups // 2)) * (key_rows // 2)
    return pl.pallas_call(
        functools.partial(attn_kernel, cfg),
        grid=(1,),
        in_specs=[q_spec] + [any_spec] * len(kv),
        out_specs=out_specs,
        out_shape=out_shape,
        scratch_shapes=scratch,
        compiler_params=pltpu.CompilerParams(vmem_limit_bytes=60 * 2**20, dimension_semantics=("arbitrary",), collective_id=1 if upper else 0, has_side_effects=True),
        cost_estimate=pl.CostEstimate(flops=rows * heads * n_keys * 4 * head_dim, bytes_accessed=16 * 2**20, transcendentals=rows * heads * n_keys),
        name="attn_upper" if upper else "attn_lower",
    )(q, *kv)


CHUNK = 256
TILE = 512
N_BUF = 3


def mlp_kernel(cfg, *refs):
    tp, n_o = cfg['tp'], cfg['n_o']
    x_ref = refs[0]
    o_refs = refs[1:1 + n_o]
    (wo_ref, gain_ref, wg_ref, wu_ref, wd_ref, out_ref, wbuf, o_buf, x_buf, y_scr, h_scr, act_scr, part, y_mine, far_buf, near_buf, mine,
     w_sem, in_sem, far_send, far_recv, near_send, near_recv, ag_send, ag_recv, fwd_send, fwd_recv, own_sem) = refs[1 + n_o:]
    rows, width = x_ref.shape
    ff = wg_ref.shape[1]
    n_chunks = rows // CHUNK
    shard = CHUNK // tp
    half = shard // 2
    n_wo, n_gu, n_dn = width // TILE, ff // (TILE // 2), width // TILE
    per = n_wo + n_gu + n_dn
    total = per * n_chunks
    my_tp = lax.axis_index('tp')
    MESH = pl.DeviceIdType.MESH
    above, below = {'tp': (my_tp + 1) % tp}, {'tp': (my_tp + tp - 1) % tp}

    barrier = pltpu.get_barrier_semaphore()
    for dev in (above, below):
        pl.semaphore_signal(barrier, inc=1, device_id=dev, device_id_type=MESH)
    pl.semaphore_wait(barrier, 2)

    def cols(i, n):
        return pl.ds(pl.multiple_of(i * n, n), n)

    def tile_copies(kind, i, slot):
        if kind == 0:
            return [pltpu.make_async_copy(wo_ref.at[:, cols(i, TILE)], wbuf.at[slot], w_sem.at[slot, 0])]
        if kind == 1:
            h = TILE // 2
            return [pltpu.make_async_copy(wg_ref.at[:, cols(i, h)], wbuf.at[slot, :, pl.ds(0, h)], w_sem.at[slot, 0]),
                    pltpu.make_async_copy(wu_ref.at[:, cols(i, h)], wbuf.at[slot, :, pl.ds(h, h)], w_sem.at[slot, 1])]
        return [pltpu.make_async_copy(wd_ref.at[:, cols(i, TILE)], wbuf.at[slot, pl.ds(0, ff)], w_sem.at[slot, 0])]

    def fetch(g):
        t = g % per
        slot = g % N_BUF
        for kind, lo, hi in ((0, 0, n_wo), (1, n_wo, n_wo + n_gu), (2, n_wo + n_gu, per)):
            @pl.when((g < total) & (t >= lo) & (t < hi))
            def _():
                for copy in tile_copies(kind, t - lo, slot):
                    copy.start()

    def tile_loop(c, kind, lo, n, use):
        def body(i, carry):
            g = c * per + lo + i
            slot = g % N_BUF
            for copy in tile_copies(kind, i, slot):
                copy.wait()
            fetch(g + N_BUF - 1)
            use(i, slot)
            return carry
        lax.fori_loop(0, n, body, 0)

    def chunk_rows(c):
        return pl.ds(pl.multiple_of(c * CHUNK, CHUNK), CHUNK)

    def input_copies(c, which):
        o_rows = rows // n_o // CHUNK
        return [pltpu.make_async_copy(x_ref.at[chunk_rows(c)], x_buf, in_sem.at[0]),
                pltpu.make_async_copy(o_refs[which].at[chunk_rows(c - which * o_rows)], o_buf, in_sem.at[1])]

    def fetch_inputs(c):
        o_rows = rows // n_o // CHUNK
        for which in range(n_o):
            @pl.when((c < n_chunks) & (c >= which * o_rows) & (c < (which + 1) * o_rows))
            def _():
                for copy in input_copies(c, which):
                    copy.start()

    def owner_rows(k, lo, n):
        return pl.ds(pl.multiple_of(((my_tp + k) % tp) * shard + lo, n), n)

    def remote(src, dst, send, recv, dev):
        return pltpu.make_async_remote_copy(src_ref=src, dst_ref=dst, send_sem=send, recv_sem=recv, device_id=dev, device_id_type=MESH)

    def far_copies(c):
        p = c % 2
        return [remote(part.at[p, owner_rows(2, 0, half)], far_buf.at[c, 0], far_send.at[c, 0], far_recv.at[c, 0], above),
                remote(part.at[p, owner_rows(2, half, half)], far_buf.at[c, 1], far_send.at[c, 1], far_recv.at[c, 1], below)]

    def near_copies(c):
        p = c % 2
        return [remote(part.at[p, owner_rows(1, 0, shard)], near_buf.at[c, 0], near_send.at[c, 0], near_recv.at[c, 0], above),
                remote(part.at[p, owner_rows(tp - 1, 0, shard)], near_buf.at[c, 1], near_send.at[c, 1], near_recv.at[c, 1], below)]

    def out_rows(c, k, lo, n):
        return out_ref.at[pl.ds(pl.multiple_of(c * CHUNK + ((my_tp + k) % tp) * shard + lo, n), n)]

    def gather_copies(c):
        dst = out_rows(c, 0, 0, shard)
        return [remote(mine.at[c], dst, ag_send.at[c, 0], ag_recv.at[c, 0], above),
                remote(mine.at[c], dst, ag_send.at[c, 1], ag_recv.at[c, 1], below)]

    def forward_copies(c):
        lower, upper = out_rows(c, tp - 1, 0, half), out_rows(c, 1, half, half)
        return [remote(lower, lower, fwd_send.at[c, 0], fwd_recv.at[c, 0], above),
                remote(upper, upper, fwd_send.at[c, 1], fwd_recv.at[c, 1], below)]

    def own_copy(c):
        return pltpu.make_async_copy(mine.at[c], out_rows(c, 0, 0, shard), own_sem.at[c])

    def send_far(c):
        for copy in far_copies(c):
            copy.start()

    def send_near(c):
        for copy in far_copies(c):
            copy.wait_recv()
        p = c % 2

        def add(i, carry):
            cs = cols(i, TILE)
            part[p, owner_rows(1, 0, half), cs] += far_buf[c, 0, :, cs]
            part[p, owner_rows(tp - 1, half, half), cs] += far_buf[c, 1, :, cs]
            return carry
        lax.fori_loop(0, width // TILE, add, 0)
        for copy in near_copies(c):
            copy.start()

    def send_result(c):
        for copy in near_copies(c):
            copy.wait_recv()
        p = c % 2

        def add(i, carry):
            cs = cols(i, TILE)
            total_rows = part[p, owner_rows(0, 0, shard), cs] + near_buf[c, 0, :, cs] + near_buf[c, 1, :, cs]
            mine[c, :, cs] = (y_mine[p, :, cs] + total_rows).astype(mine.dtype)
            return carry
        lax.fori_loop(0, width // TILE, add, 0)
        own_copy(c).start()
        for copy in gather_copies(c):
            copy.start()
        for copy in far_copies(c) + near_copies(c):
            copy.wait_send()

    def forward_result(c):
        for copy in gather_copies(c):
            copy.wait_recv()
        for copy in forward_copies(c):
            copy.start()

    fetch_inputs(0)
    for g in range(N_BUF - 1):
        fetch(g)

    def chunk_body(c, carry):
        p = c % 2
        for copy in input_copies(0, 0):
            copy.wait()

        def proj(i, slot):
            cs = cols(i, TILE)
            y_scr[:, cs] = x_buf[:, cs].astype(jnp.float32) + jnp.dot(o_buf[...], wbuf[slot], preferred_element_type=jnp.float32)

        tile_loop(c, 0, 0, n_wo, proj)
        fetch_inputs(c + 1)

        def square(i, acc):
            y = y_scr[:, cols(i, TILE)]
            y2 = y * y
            for k in range(TILE // 128):
                acc = acc + y2[:, k * 128:(k + 1) * 128]
            return acc
        acc = lax.fori_loop(0, width // TILE, square, jnp.zeros((CHUNK, 128), jnp.float32))
        inv_rms = lax.rsqrt(jnp.sum(acc, axis=1, keepdims=True) / width + NORM_EPS)

        def norm(i, carry):
            cs = cols(i, TILE)
            h_scr[:, cs] = (y_scr[:, cs] * inv_rms * gain_ref[:, cs].astype(jnp.float32)).astype(h_scr.dtype)
            y_mine[p, :, cs] = y_scr[owner_rows(0, 0, shard), cs]
            return carry
        lax.fori_loop(0, width // TILE, norm, 0)

        @pl.when(c > 0)
        def _():
            send_near(c - 1)

        @pl.when(c > 1)
        def _():
            forward_result(c - 2)

        def gated(i, slot):
            gu = jnp.dot(h_scr[...], wbuf[slot], preferred_element_type=jnp.float32)
            gate, up = gu[:, :TILE // 2], gu[:, TILE // 2:]
            act_scr[:, cols(i, TILE // 2)] = (gate * lax.logistic(gate) * up).astype(act_scr.dtype)

        tile_loop(c, 1, n_wo, n_gu, gated)

        @pl.when(c > 0)
        def _():
            send_result(c - 1)

        def down(i, slot):
            part[p, :, cols(i, TILE)] = jnp.dot(act_scr[...], wbuf[slot, :ff], preferred_element_type=jnp.float32)

        tile_loop(c, 2, n_wo + n_gu, n_dn, down)
        send_far(c)
        return carry

    lax.fori_loop(0, n_chunks, chunk_body, 0)
    send_near(n_chunks - 1)
    forward_result(n_chunks - 2)
    send_result(n_chunks - 1)
    forward_result(n_chunks - 1)

    def drain(c, carry):
        own_copy(c).wait()
        for copy in gather_copies(c):
            copy.wait_send()
        for copy in forward_copies(c):
            copy.wait()
        return carry
    lax.fori_loop(0, n_chunks, drain, 0)


def mlp_block(x, o_parts, w_out, gain, w_gate, w_up, w_down, tp):
    rows, width = x.shape
    ff = w_gate.shape[1]
    n = rows // CHUNK
    shard = CHUNK // tp
    any_spec = pl.BlockSpec(memory_space=pl.ANY)
    bf, f32, dma = jnp.bfloat16, jnp.float32, pltpu.SemaphoreType.DMA
    pair = dma((n, 2))
    scratch = [pltpu.VMEM((N_BUF, width, TILE), bf), pltpu.VMEM((CHUNK, width), bf), pltpu.VMEM((CHUNK, width), bf), pltpu.VMEM((CHUNK, width), f32),
               pltpu.VMEM((CHUNK, width), bf), pltpu.VMEM((CHUNK, ff), bf), pltpu.VMEM((2, CHUNK, width), f32), pltpu.VMEM((2, shard, width), f32),
               pltpu.VMEM((n, 2, shard // 2, width), f32), pltpu.VMEM((n, 2, shard, width), f32), pltpu.VMEM((n, shard, width), bf),
               dma((N_BUF, 2)), dma((2,)), pair, pair, pair, pair, pair, pair, pair, pair, dma((n,))]
    flops = 2 * rows * width * (w_out.shape[0] + 3 * ff)
    return pl.pallas_call(
        functools.partial(mlp_kernel, dict(tp=tp, n_o=len(o_parts))),
        grid=(1,),
        in_specs=[any_spec] * (2 + len(o_parts)) + [pl.BlockSpec((1, width), lambda i: (0, 0))] + [any_spec] * 3,
        out_specs=any_spec,
        out_shape=jax.ShapeDtypeStruct(x.shape, x.dtype),
        scratch_shapes=scratch,
        compiler_params=pltpu.CompilerParams(vmem_limit_bytes=63 * 2**20, dimension_semantics=("arbitrary",), collective_id=2, has_side_effects=True),
        cost_estimate=pl.CostEstimate(flops=flops, bytes_accessed=500 * 2**20, transcendentals=rows * ff),
        name="mlp",
    )(x, *o_parts, w_out, gain.reshape(1, width), w_gate, w_up, w_down)


def solution(mesh):
    groups = mesh.shape['cp']
    tp = mesh.shape['tp']

    def local_layer(x_loc, kp_loc, vp_loc, norm_attn, w_query, w_key, w_value, w_out, norm_mlp, w_gate, w_up, w_down):
        rows_loc = x_loc.shape[0]
        blk_len = rows_loc // 2
        pre_dev, kv_loc, head_dim = kp_loc.shape
        heads_loc = w_query.shape[1] // head_dim
        prefix_len = pre_dev * groups
        my_cp = lax.axis_index('cp')

        def bundle_of(k, v):
            kt = jnp.moveaxis(k, 1, 0)
            vt = v.reshape(rows_loc // head_dim, head_dim, kv_loc, head_dim).transpose(2, 0, 3, 1).reshape(kv_loc, rows_loc, head_dim)
            return jnp.concatenate([kt, vt], axis=1)

        w_rows = w_out.shape[0] // groups
        w_out_full = lax.all_gather(lax.dynamic_slice_in_dim(w_out, my_cp * w_rows, w_rows, 0), ('tp', 'cp'), tiled=True)

        local_row = jnp.arange(rows_loc, dtype=jnp.int32)
        blk_idx = jnp.where(local_row < blk_len, my_cp, 2 * groups - 1 - my_cp)
        q_pos = prefix_len + blk_idx * blk_len + local_row % blk_len
        cos_tab, sin_tab = rope_tables(q_pos, head_dim)
        hidden = rms_norm(x_loc, norm_attn)
        k_proj = jnp.dot(hidden, w_key, preferred_element_type=jnp.float32).reshape(rows_loc, kv_loc, head_dim)
        k_new = apply_rope(k_proj, cos_tab, sin_tab).astype(jnp.bfloat16)
        v_new = jnp.dot(hidden, w_value, preferred_element_type=jnp.float32).astype(jnp.bfloat16).reshape(rows_loc, kv_loc, head_dim)
        q_proj = jnp.dot(hidden, w_query, preferred_element_type=jnp.float32).reshape(rows_loc, heads_loc, head_dim)
        q_rot = apply_rope(q_proj, cos_tab, sin_tab).astype(jnp.bfloat16).reshape(rows_loc, heads_loc * head_dim)

        cfg = dict(groups=groups, tp=tp, kv_heads=kv_loc, ratio=heads_loc // kv_loc, head_dim=head_dim, key_rows=rows_loc, rows=blk_len)
        o_a, kv_all = attention(q_rot, [bundle_of(kp_loc, vp_loc), bundle_of(k_new, v_new)], dict(cfg, ring=True, upper=False))

        o_b = attention(q_rot, [kv_all], dict(cfg, ring=False, upper=True))
        x_out = mlp_block(x_loc, [o_a, o_b], w_out_full, norm_mlp, w_gate, w_up, w_down, tp)
        return x_out, k_new, v_new

    row_spec = P(('dp', 'cp'), None)
    kv_spec = P(('dp', 'cp'), 'tp', None)
    col_spec = P(None, 'tp')
    row_split = P('tp', None)
    vec_spec = P(None)
    return jax.shard_map(local_layer, mesh=mesh, in_specs=(row_spec, kv_spec, kv_spec, vec_spec, col_spec, col_spec, col_spec, row_split, vec_spec, col_spec, col_spec, row_split), out_specs=(row_spec, kv_spec, kv_spec), check_vma=False)
```

```python
import functools

import jax
import jax.numpy as jnp
from jax import lax
from jax.experimental import pallas as pl
from jax.experimental.pallas import tpu as pltpu
from jax.sharding import PartitionSpec as P

ROPE_THETA = 500000.0
NORM_EPS = 1e-5
LOG2E = 1.4426950408889634
KEY_BLOCK = 512


def rope_tables(positions, head_dim):
    inv_freq = ROPE_THETA ** (-jnp.arange(0, head_dim, 2, dtype=jnp.float32) / head_dim)
    angles = positions.astype(jnp.float32)[:, None] * inv_freq[None, :]
    return jnp.cos(angles), jnp.sin(angles)


def apply_rope(values, cos_tab, sin_tab):
    half_dim = values.shape[-1] // 2
    first_half = values[..., :half_dim]
    second_half = values[..., half_dim:]
    cos_rows = cos_tab[:, None, :]
    sin_rows = sin_tab[:, None, :]
    return jnp.concatenate([first_half * cos_rows - second_half * sin_rows, second_half * cos_rows + first_half * sin_rows], axis=-1)


def rms_norm(values, gain_vec):
    vals32 = values.astype(jnp.float32)
    inv_rms = lax.rsqrt(jnp.mean(vals32 * vals32, axis=-1, keepdims=True) + NORM_EPS)
    return (vals32 * inv_rms * gain_vec.astype(jnp.float32)).astype(jnp.bfloat16)


def attn_kernel(cfg, *refs):
    groups, tp, kv_heads, ratio, head_dim, key_rows, rows = (cfg[k] for k in ('groups', 'tp', 'kv_heads', 'ratio', 'head_dim', 'key_rows', 'rows'))
    heads = kv_heads * ratio
    (q_raw, cos_ref, sin_ref, pre_ref, suf_ref, w_ref, o_full, w_full, q_ref, kv_scr, s_scr, o_scr, st_scr, kv_send, kv_recv, o_send, o_recv, o_local,
     wn_send, wn_recv, wf_send, wf_recv, wx_send, wx_recv, ws_send, ws_recv) = refs
    me, my_tp = lax.axis_index('cp'), lax.axis_index('tp')
    my_x, my_core = me // 2, me % 2
    half = key_rows // 2
    scale = (head_dim ** -0.5) * LOG2E
    MESH = pl.DeviceIdType.MESH
    sib = {'cp': my_x * 2 + (1 - my_core)}
    x_next = {'cp': (me + 2) % groups}
    x_prev = {'cp': (me + groups - 2) % groups}
    peers = [{'tp': (my_tp + k) % tp} for k in range(1, tp)]

    barrier = pltpu.get_barrier_semaphore()
    greet = peers + [sib, x_next, x_prev]
    for dev in greet:
        pl.semaphore_signal(barrier, inc=1, device_id=dev, device_id_type=MESH)
    pl.semaphore_wait(barrier, len(greet))

    def kv_copy(part, g, slot):
        base = part * groups
        src_own = (pre_ref, suf_ref)[part].at[g]
        dst = kv_scr.at[g, base + slot]
        if slot == 0:
            return pltpu.make_async_copy(src_own, dst, kv_recv.at[g, base])
        if slot in (1, 2, 3):
            src = src_own
        elif slot in (4, 5):
            src = kv_scr.at[g, base + slot - 2]
        elif slot == 6:
            src = kv_scr.at[g, base + (2 if g == 0 else 3)]
        else:
            src = kv_scr.at[g, base + 6]
        dev = {1: sib, 4: sib, 5: sib, 7: sib, 2: x_next, 3: x_prev, 6: x_next if g == 0 else x_prev}[slot]
        return pltpu.make_async_remote_copy(src_ref=src, dst_ref=dst, send_sem=kv_send.at[g, base + slot], recv_sem=kv_recv.at[g, base + slot], device_id=dev, device_id_type=MESH)

    gs = range(kv_heads)

    def start(part, slots):
        for slot in slots:
            for g in gs:
                kv_copy(part, g, slot).start()

    def arrived(part, slots):
        for slot in slots:
            for g in gs:
                copy = kv_copy(part, g, slot)
                copy.wait() if slot == 0 else copy.wait_recv()

    n_pre = 2 * groups

    quarter = w_ref.shape[0] // 4
    w_half = quarter // 2
    my_quarter = 2 * (my_x % 2) + my_core
    x_quarter = 2 * (1 - my_x % 2) + my_core
    above, below = {'tp': (my_tp + 1) % tp}, {'tp': (my_tp + tp - 1) % tp}
    ks = (tp - 1, 1, 2)

    def w_rows(k, which, lo, n):
        return w_full.at[pl.ds(pl.multiple_of(((my_tp + k) % tp) * w_ref.shape[0] + which * quarter + lo, n), n)]

    def remote(src, dst, send, recv, dev):
        return pltpu.make_async_remote_copy(src_ref=src, dst_ref=dst, send_sem=send, recv_sem=recv, device_id=dev, device_id_type=MESH)

    def w_near():
        src = w_ref.at[pl.ds(pl.multiple_of(my_quarter * quarter, quarter), quarter)]
        return [remote(src, w_rows(0, my_quarter, 0, quarter), wn_send.at[i], wn_recv.at[i], dev) for i, dev in enumerate((above, below))]

    def w_far():
        out = []
        for i, (k, dev) in enumerate(((tp - 1, above), (1, below))):
            piece = w_rows(k, my_quarter, i * w_half, w_half)
            out.append(remote(piece, piece, wf_send.at[i], wf_recv.at[i], dev))
        return out

    def w_x(n):
        out = []
        for i, dev in enumerate((x_next, x_prev)):
            piece = w_rows(ks[n], my_quarter, i * w_half, w_half)
            out.append(remote(piece, piece, wx_send.at[i, n], wx_recv.at[i, n], dev))
        return out

    def w_sib(n, second):
        piece = w_rows(ks[n], x_quarter if second else my_quarter, 0, quarter)
        return remote(piece, piece, ws_send.at[int(second), n], ws_recv.at[int(second), n], sib)

    def rope(h, carry):
        cs = pl.ds(pl.multiple_of(h * head_dim, head_dim), head_dim)
        x = q_raw[:, cs]
        q_ref[:, cs] = (x * cos_ref[...] + pltpu.roll(x, head_dim // 2, 1) * sin_ref[...]).astype(q_ref.dtype)
        return carry

    def locate(j):
        b = j - n_pre
        lower = b < groups
        dev = jnp.where(lower, b, 2 * groups - 1 - b)
        rel = (dev // 2 - my_x + groups // 2) % (groups // 2)
        same = dev % 2 == my_core
        s_slot = jnp.where(rel == 0, jnp.where(same, 0, 1), jnp.where(rel == 1, jnp.where(same, 3, 5), jnp.where(rel == 2, jnp.where(same, 6, 7), jnp.where(same, 2, 4))))
        pre = j < n_pre
        return jnp.where(pre, j // 2, groups + s_slot), jnp.where(pre, (j % 2) * half, jnp.where(lower, 0, half))

    def head_pass(upper, h, lo, hi, suffix, load, store):
        g = h // ratio
        blk = (2 * groups - 1 - me) if upper else me
        q = q_ref[upper * rows:(upper + 1) * rows, pl.ds(pl.multiple_of(h * head_dim, head_dim), head_dim)]

        def scores(j):
            slot, off = locate(j)
            k = kv_scr[g, slot, pl.ds(pl.multiple_of(off, half), half), :]
            return lax.dot_general(k, q, (((1,), (1,)), ((), ())), preferred_element_type=jnp.float32)

        def values_t(j):
            slot, off = locate(j)
            v = kv_scr[g, slot, pl.ds(pl.multiple_of(key_rows + off, half), half), :]
            return jnp.concatenate([v[i * head_dim:(i + 1) * head_dim] for i in range(half // head_dim)], axis=1)

        def update(s, v, state):
            m, l, acc = state
            n = s.shape[0]
            folded = jnp.max(s.reshape(n // 8, 8, rows), axis=0)
            m_new = jnp.maximum(m, jnp.max(folded, axis=0, keepdims=True))
            a = jnp.exp2((m - m_new) * scale)
            p = jnp.exp2(s * scale - m_new * scale)
            l = l * a + jnp.sum(p.reshape(n // 8, 8, rows), axis=0)
            acc = acc * a + jnp.dot(v, p.astype(jnp.bfloat16), preferred_element_type=jnp.float32)
            return m_new, l, acc

        last = n_pre + blk if suffix else hi - 1
        if load:
            state = (st_scr[h, head_dim + 8:head_dim + 9], st_scr[h, head_dim:head_dim + 8], st_scr[h, :head_dim])
        else:
            state = (jnp.full((1, rows), -jnp.inf, jnp.float32), jnp.zeros((8, rows), jnp.float32), jnp.zeros((head_dim, rows), jnp.float32))
        s_scr[0] = scores(lo)

        def make_body(base, unroll):
            def body(i, st):
                for u in range(unroll):
                    j = base + i * unroll + u
                    s_scr[(u + 1) % 2] = scores(jnp.minimum(j + 1, last))
                    st = update(s_scr[u % 2], values_t(j), st)
                return st
            return body

        state = lax.fori_loop(0, (hi - lo) // 4, make_body(lo, 4), state)
        if suffix:
            state = lax.fori_loop(0, blk // 2, make_body(n_pre, 2), state)

            def odd_body(i, st):
                s_scr[1] = scores(last)
                return update(s_scr[0], values_t(last - 1), st)

            state = lax.fori_loop(0, blk % 2, odd_body, state)
            s = s_scr[blk % 2]
            kid = lax.broadcasted_iota(jnp.int32, s.shape, 0)
            qid = lax.broadcasted_iota(jnp.int32, s.shape, 1)
            state = update(jnp.where(kid <= qid, s, -jnp.inf), values_t(last), state)
        m, l, acc = state
        if store:
            st_scr[h, :head_dim] = acc
            st_scr[h, head_dim:head_dim + 8] = l
            st_scr[h, head_dim + 8:] = jnp.broadcast_to(m, (8, rows))
        else:
            o_scr[upper * heads + h] = (acc / jnp.sum(l, axis=0, keepdims=True)).T.astype(o_scr.dtype)

    def o_dst(upper, h):
        return o_full.at[upper * rows:(upper + 1) * rows, pl.ds(pl.multiple_of(my_tp * heads * head_dim + h * head_dim, head_dim), head_dim)]

    def o_copies(upper, h):
        i = upper * heads + h
        return [remote(o_scr.at[i], o_dst(upper, h), o_send.at[k, i], o_recv.at[k, i], dev) for k, dev in enumerate(peers)]

    def o_own(upper, h):
        return pltpu.make_async_copy(o_scr.at[upper * heads + h], o_dst(upper, h), o_local.at[upper * heads + h])

    def loop_heads(upper, lo_h, hi_h, lo, hi, suffix, load):
        def body(h, carry):
            head_pass(upper, h, lo, hi, suffix, load, not suffix)
            if suffix:
                o_own(upper, h).start()
                for copy in o_copies(upper, h):
                    copy.start()
            return carry
        lax.fori_loop(lo_h, hi_h, body, 0)

    start(0, (0, 1, 2, 3))
    for copy in w_near():
        copy.start()
    start(1, (0, 1, 2, 3))
    lax.fori_loop(0, heads, rope, 0)
    arrived(0, (0, 1))
    loop_heads(0, 0, heads, 0, 4, False, False)
    arrived(0, (2, 3))
    start(0, (4, 5, 6))
    loop_heads(0, 0, heads, 4, 8, False, True)
    arrived(0, (4, 5))
    loop_heads(0, 0, heads, 8, 12, False, True)
    arrived(0, (6,))
    start(0, (7,))
    arrived(1, (0, 1, 2, 3))
    start(1, (4, 5, 6))
    for copy in w_near():
        copy.wait_recv()
    for copy in w_far():
        copy.start()
    arrived(0, (7,))
    arrived(1, (4, 5, 6))
    start(1, (7,))
    for n in range(2):
        w_sib(n, False).start()
        for copy in w_x(n):
            copy.start()
    arrived(1, (7,))
    loop_heads(0, 0, heads, 12, 16, True, True)
    for copy in w_far():
        copy.wait_recv()
    w_sib(2, False).start()
    for copy in w_x(2):
        copy.start()
    loop_heads(1, 0, heads // 2, 0, 16, True, False)
    for n in range(3):
        for copy in w_x(n):
            copy.wait_recv()
        w_sib(n, True).start()
    loop_heads(1, heads // 2, heads, 0, 16, True, False)

    for g in gs:
        for part in range(2):
            for slot in range(1, groups):
                kv_copy(part, g, slot).wait_send()
    for copy in w_near() + w_far():
        copy.wait_send()
    for n in range(3):
        for copy in w_x(n):
            copy.wait_send()
        for second in (False, True):
            w_sib(n, second).wait()

    for upper in range(2):
        def drain(h, carry):
            o_own(upper, h).wait()
            for copy in o_copies(upper, h):
                copy.wait()
            return carry
        lax.fori_loop(0, heads, drain, 0)


def attention(q, cos, sin, pre, suf, w_out, cfg):
    groups, tp, kv_heads, ratio, head_dim, key_rows, rows = (cfg[k] for k in ('groups', 'tp', 'kv_heads', 'ratio', 'head_dim', 'key_rows', 'rows'))
    heads = kv_heads * ratio
    bf, f32, dma = jnp.bfloat16, jnp.float32, pltpu.SemaphoreType.DMA
    any_spec = pl.BlockSpec(memory_space=pl.ANY)
    whole = lambda arr: pl.BlockSpec(arr.shape, lambda i: (0, 0))
    kv_shape = (kv_heads, 2 * groups, 2 * key_rows, head_dim)
    kv_sem, o_sem = dma((kv_heads, 2 * groups)), dma((tp - 1, 2 * heads))
    scratch = [pltpu.VMEM(q.shape, bf), pltpu.VMEM(kv_shape, bf), pltpu.VMEM((2, key_rows // 2, rows), f32), pltpu.VMEM((2 * heads, rows, head_dim), bf),
               pltpu.VMEM((heads, head_dim + 16, rows), f32), kv_sem, kv_sem, o_sem, o_sem, dma((2 * heads,)),
               dma((2,)), dma((2,)), dma((2,)), dma((2,)), dma((2, 3)), dma((2, 3)), dma((2, 3)), dma((2, 3))]
    n_keys = (4 * groups + 2 * groups) * (key_rows // 2)
    return pl.pallas_call(
        functools.partial(attn_kernel, cfg),
        grid=(1,),
        in_specs=[whole(q), whole(cos), whole(sin)] + [any_spec] * 3,
        out_specs=(any_spec, any_spec),
        out_shape=(jax.ShapeDtypeStruct((2 * rows, tp * heads * head_dim), bf), jax.ShapeDtypeStruct((tp * w_out.shape[0], w_out.shape[1]), bf)),
        scratch_shapes=scratch,
        compiler_params=pltpu.CompilerParams(vmem_limit_bytes=60 * 2**20, dimension_semantics=("arbitrary",), collective_id=0, has_side_effects=True),
        cost_estimate=pl.CostEstimate(flops=rows * heads * n_keys * 4 * head_dim, bytes_accessed=16 * 2**20, transcendentals=rows * heads * n_keys),
        name="attn",
    )(q, cos, sin, pre, suf, w_out)


CHUNK = 256
TILE = 512
N_BUF = 3


def mlp_kernel(cfg, *refs):
    tp, n_o = cfg['tp'], cfg['n_o']
    x_ref = refs[0]
    o_refs = refs[1:1 + n_o]
    (wo_ref, wown_ref, gain_ref, wg_ref, wu_ref, wd_ref, out_ref, wbuf, o_buf, x_buf, y_scr, h_scr, act_scr, part, y_mine, far_buf, near_buf, mine,
     w_sem, in_sem, far_send, far_recv, near_send, near_recv, ag_send, ag_recv, fwd_send, fwd_recv, own_sem) = refs[1 + n_o:]
    rows, width = x_ref.shape
    ff = wg_ref.shape[1]
    n_chunks = rows // CHUNK
    shard = CHUNK // tp
    half = shard // 2
    n_wo, n_gu, n_dn = width // TILE, ff // (TILE // 2), width // TILE
    per = n_wo + n_gu + n_dn
    total = per * n_chunks
    my_tp = lax.axis_index('tp')
    MESH = pl.DeviceIdType.MESH
    above, below = {'tp': (my_tp + 1) % tp}, {'tp': (my_tp + tp - 1) % tp}

    barrier = pltpu.get_barrier_semaphore()
    for dev in (above, below):
        pl.semaphore_signal(barrier, inc=1, device_id=dev, device_id_type=MESH)
    pl.semaphore_wait(barrier, 2)

    def cols(i, n):
        return pl.ds(pl.multiple_of(i * n, n), n)

    def tile_copies(kind, i, slot):
        if kind == 0:
            n = wown_ref.shape[0]
            out = []
            for k in range(tp):
                part_rows = pl.ds(pl.multiple_of(((my_tp + k) % tp) * n, n), n)
                src = wo_ref.at[part_rows, cols(i, TILE)] if k else wown_ref.at[:, cols(i, TILE)]
                out.append(pltpu.make_async_copy(src, wbuf.at[slot, part_rows], w_sem.at[slot, k]))
            return out
        if kind == 1:
            h = TILE // 2
            return [pltpu.make_async_copy(wg_ref.at[:, cols(i, h)], wbuf.at[slot, :, pl.ds(0, h)], w_sem.at[slot, 0]),
                    pltpu.make_async_copy(wu_ref.at[:, cols(i, h)], wbuf.at[slot, :, pl.ds(h, h)], w_sem.at[slot, 1])]
        return [pltpu.make_async_copy(wd_ref.at[:, cols(i, TILE)], wbuf.at[slot, pl.ds(0, ff)], w_sem.at[slot, 0])]

    def fetch(g):
        t = g % per
        slot = g % N_BUF
        for kind, lo, hi in ((0, 0, n_wo), (1, n_wo, n_wo + n_gu), (2, n_wo + n_gu, per)):
            @pl.when((g < total) & (t >= lo) & (t < hi))
            def _():
                for copy in tile_copies(kind, t - lo, slot):
                    copy.start()

    def tile_loop(c, kind, lo, n, use):
        def body(i, carry):
            g = c * per + lo + i
            slot = g % N_BUF
            for copy in tile_copies(kind, i, slot):
                copy.wait()
            fetch(g + N_BUF - 1)
            use(i, slot)
            return carry
        lax.fori_loop(0, n, body, 0)

    def chunk_rows(c):
        return pl.ds(pl.multiple_of(c * CHUNK, CHUNK), CHUNK)

    def input_copies(c, which):
        o_rows = rows // n_o // CHUNK
        return [pltpu.make_async_copy(x_ref.at[chunk_rows(c)], x_buf, in_sem.at[0]),
                pltpu.make_async_copy(o_refs[which].at[chunk_rows(c - which * o_rows)], o_buf, in_sem.at[1])]

    def fetch_inputs(c):
        o_rows = rows // n_o // CHUNK
        for which in range(n_o):
            @pl.when((c < n_chunks) & (c >= which * o_rows) & (c < (which + 1) * o_rows))
            def _():
                for copy in input_copies(c, which):
                    copy.start()

    def owner_rows(k, lo, n):
        return pl.ds(pl.multiple_of(((my_tp + k) % tp) * shard + lo, n), n)

    def remote(src, dst, send, recv, dev):
        return pltpu.make_async_remote_copy(src_ref=src, dst_ref=dst, send_sem=send, recv_sem=recv, device_id=dev, device_id_type=MESH)

    def far_copies(c):
        p = c % 2
        return [remote(part.at[p, owner_rows(2, 0, half)], far_buf.at[c, 0], far_send.at[c, 0], far_recv.at[c, 0], above),
                remote(part.at[p, owner_rows(2, half, half)], far_buf.at[c, 1], far_send.at[c, 1], far_recv.at[c, 1], below)]

    def near_copies(c):
        p = c % 2
        return [remote(part.at[p, owner_rows(1, 0, shard)], near_buf.at[c, 0], near_send.at[c, 0], near_recv.at[c, 0], above),
                remote(part.at[p, owner_rows(tp - 1, 0, shard)], near_buf.at[c, 1], near_send.at[c, 1], near_recv.at[c, 1], below)]

    def out_rows(c, k, lo, n):
        return out_ref.at[pl.ds(pl.multiple_of(c * CHUNK + ((my_tp + k) % tp) * shard + lo, n), n)]

    def gather_copies(c):
        dst = out_rows(c, 0, 0, shard)
        return [remote(mine.at[c], dst, ag_send.at[c, 0], ag_recv.at[c, 0], above),
                remote(mine.at[c], dst, ag_send.at[c, 1], ag_recv.at[c, 1], below)]

    def forward_copies(c):
        lower, upper = out_rows(c, tp - 1, 0, half), out_rows(c, 1, half, half)
        return [remote(lower, lower, fwd_send.at[c, 0], fwd_recv.at[c, 0], above),
                remote(upper, upper, fwd_send.at[c, 1], fwd_recv.at[c, 1], below)]

    def own_copy(c):
        return pltpu.make_async_copy(mine.at[c], out_rows(c, 0, 0, shard), own_sem.at[c])

    def send_far(c):
        for copy in far_copies(c):
            copy.start()

    def send_near(c):
        for copy in far_copies(c):
            copy.wait_recv()
        p = c % 2

        def add(i, carry):
            cs = cols(i, TILE)
            part[p, owner_rows(1, 0, half), cs] += far_buf[c, 0, :, cs]
            part[p, owner_rows(tp - 1, half, half), cs] += far_buf[c, 1, :, cs]
            return carry
        lax.fori_loop(0, width // TILE, add, 0)
        for copy in near_copies(c):
            copy.start()

    def send_result(c):
        for copy in near_copies(c):
            copy.wait_recv()
        p = c % 2

        def add(i, carry):
            cs = cols(i, TILE)
            total_rows = part[p, owner_rows(0, 0, shard), cs] + near_buf[c, 0, :, cs] + near_buf[c, 1, :, cs]
            mine[c, :, cs] = (y_mine[p, :, cs] + total_rows).astype(mine.dtype)
            return carry
        lax.fori_loop(0, width // TILE, add, 0)
        own_copy(c).start()
        for copy in gather_copies(c):
            copy.start()
        for copy in far_copies(c) + near_copies(c):
            copy.wait_send()

    def forward_result(c):
        for copy in gather_copies(c):
            copy.wait_recv()
        for copy in forward_copies(c):
            copy.start()

    fetch_inputs(0)
    for g in range(N_BUF - 1):
        fetch(g)

    def chunk_body(c, carry):
        p = c % 2
        for copy in input_copies(0, 0):
            copy.wait()

        def proj(i, slot):
            cs = cols(i, TILE)
            y_scr[:, cs] = x_buf[:, cs].astype(jnp.float32) + jnp.dot(o_buf[...], wbuf[slot], preferred_element_type=jnp.float32)

        tile_loop(c, 0, 0, n_wo, proj)
        fetch_inputs(c + 1)

        def square(i, acc):
            y = y_scr[:, cols(i, TILE)]
            y2 = y * y
            for k in range(TILE // 128):
                acc = acc + y2[:, k * 128:(k + 1) * 128]
            return acc
        acc = lax.fori_loop(0, width // TILE, square, jnp.zeros((CHUNK, 128), jnp.float32))
        inv_rms = lax.rsqrt(jnp.sum(acc, axis=1, keepdims=True) / width + NORM_EPS)

        def norm(i, carry):
            cs = cols(i, TILE)
            h_scr[:, cs] = (y_scr[:, cs] * inv_rms * gain_ref[:, cs].astype(jnp.float32)).astype(h_scr.dtype)
            y_mine[p, :, cs] = y_scr[owner_rows(0, 0, shard), cs]
            return carry
        lax.fori_loop(0, width // TILE, norm, 0)

        @pl.when(c > 0)
        def _():
            send_near(c - 1)

        @pl.when(c > 1)
        def _():
            forward_result(c - 2)

        def gated(i, slot):
            gu = jnp.dot(h_scr[...], wbuf[slot], preferred_element_type=jnp.float32)
            gate, up = gu[:, :TILE // 2], gu[:, TILE // 2:]
            act_scr[:, cols(i, TILE // 2)] = (gate * lax.logistic(gate) * up).astype(act_scr.dtype)

        tile_loop(c, 1, n_wo, n_gu, gated)

        @pl.when(c > 0)
        def _():
            send_result(c - 1)

        def down(i, slot):
            part[p, :, cols(i, TILE)] = jnp.dot(act_scr[...], wbuf[slot, :ff], preferred_element_type=jnp.float32)

        tile_loop(c, 2, n_wo + n_gu, n_dn, down)
        send_far(c)
        return carry

    lax.fori_loop(0, n_chunks, chunk_body, 0)
    send_near(n_chunks - 1)
    forward_result(n_chunks - 2)
    send_result(n_chunks - 1)
    forward_result(n_chunks - 1)

    def drain(c, carry):
        own_copy(c).wait()
        for copy in gather_copies(c):
            copy.wait_send()
        for copy in forward_copies(c):
            copy.wait()
        return carry
    lax.fori_loop(0, n_chunks, drain, 0)


def mlp_block(x, o_parts, w_out, w_own, gain, w_gate, w_up, w_down, tp):
    rows, width = x.shape
    ff = w_gate.shape[1]
    n = rows // CHUNK
    shard = CHUNK // tp
    any_spec = pl.BlockSpec(memory_space=pl.ANY)
    bf, f32, dma = jnp.bfloat16, jnp.float32, pltpu.SemaphoreType.DMA
    pair = dma((n, 2))
    scratch = [pltpu.VMEM((N_BUF, width, TILE), bf), pltpu.VMEM((CHUNK, width), bf), pltpu.VMEM((CHUNK, width), bf), pltpu.VMEM((CHUNK, width), f32),
               pltpu.VMEM((CHUNK, width), bf), pltpu.VMEM((CHUNK, ff), bf), pltpu.VMEM((2, CHUNK, width), f32), pltpu.VMEM((2, shard, width), f32),
               pltpu.VMEM((n, 2, shard // 2, width), f32), pltpu.VMEM((n, 2, shard, width), f32), pltpu.VMEM((n, shard, width), bf),
               dma((N_BUF, tp)), dma((2,)), pair, pair, pair, pair, pair, pair, pair, pair, dma((n,))]
    flops = 2 * rows * width * (w_out.shape[0] + 3 * ff)
    return pl.pallas_call(
        functools.partial(mlp_kernel, dict(tp=tp, n_o=len(o_parts))),
        grid=(1,),
        in_specs=[any_spec] * (3 + len(o_parts)) + [pl.BlockSpec((1, width), lambda i: (0, 0))] + [any_spec] * 3,
        out_specs=any_spec,
        out_shape=jax.ShapeDtypeStruct(x.shape, x.dtype),
        scratch_shapes=scratch,
        compiler_params=pltpu.CompilerParams(vmem_limit_bytes=63 * 2**20, dimension_semantics=("arbitrary",), collective_id=2, has_side_effects=True),
        cost_estimate=pl.CostEstimate(flops=flops, bytes_accessed=500 * 2**20, transcendentals=rows * ff),
        name="mlp",
    )(x, *o_parts, w_out, w_own, gain.reshape(1, width), w_gate, w_up, w_down)


def solution(mesh):
    groups = mesh.shape['cp']
    tp = mesh.shape['tp']

    def local_layer(x_loc, kp_loc, vp_loc, norm_attn, w_query, w_key, w_value, w_out, norm_mlp, w_gate, w_up, w_down):
        rows_loc = x_loc.shape[0]
        blk_len = rows_loc // 2
        pre_dev, kv_loc, head_dim = kp_loc.shape
        heads_loc = w_query.shape[1] // head_dim
        prefix_len = pre_dev * groups
        my_cp = lax.axis_index('cp')

        def bundle_of(k, v):
            kt = jnp.moveaxis(k, 1, 0)
            vt = v.reshape(rows_loc // head_dim, head_dim, kv_loc, head_dim).transpose(2, 0, 3, 1).reshape(kv_loc, rows_loc, head_dim)
            return jnp.concatenate([kt, vt], axis=1)

        local_row = jnp.arange(rows_loc, dtype=jnp.int32)
        blk_idx = jnp.where(local_row < blk_len, my_cp, 2 * groups - 1 - my_cp)
        q_pos = prefix_len + blk_idx * blk_len + local_row % blk_len
        cos_tab, sin_tab = rope_tables(q_pos, head_dim)
        hidden = rms_norm(x_loc, norm_attn)
        k_proj = jnp.dot(hidden, w_key, preferred_element_type=jnp.float32).reshape(rows_loc, kv_loc, head_dim)
        k_new = apply_rope(k_proj, cos_tab, sin_tab).astype(jnp.bfloat16)
        v_new = jnp.dot(hidden, w_value, preferred_element_type=jnp.float32).astype(jnp.bfloat16).reshape(rows_loc, kv_loc, head_dim)
        q_proj = jnp.dot(hidden, w_query, preferred_element_type=jnp.float32)
        cos_all = jnp.concatenate([cos_tab, cos_tab], axis=1)
        sin_all = jnp.concatenate([-sin_tab, sin_tab], axis=1)

        cfg = dict(groups=groups, tp=tp, kv_heads=kv_loc, ratio=heads_loc // kv_loc, head_dim=head_dim, key_rows=rows_loc, rows=blk_len)
        o_full, w_full = attention(q_proj, cos_all, sin_all, bundle_of(kp_loc, vp_loc), bundle_of(k_new, v_new), w_out, cfg)
        x_out = mlp_block(x_loc, [o_full], w_full, w_out, norm_mlp, w_gate, w_up, w_down, tp)
        return x_out, k_new, v_new

    row_spec = P(('dp', 'cp'), None)
    kv_spec = P(('dp', 'cp'), 'tp', None)
    col_spec = P(None, 'tp')
    row_split = P('tp', None)
    vec_spec = P(None)
    return jax.shard_map(local_layer, mesh=mesh, in_specs=(row_spec, kv_spec, kv_spec, vec_spec, col_spec, col_spec, col_spec, row_split, vec_spec, col_spec, col_spec, row_split), out_specs=(row_spec, kv_spec, kv_spec), check_vma=False)
```

```python
import functools

import jax
import jax.numpy as jnp
from jax import lax
from jax.experimental import pallas as pl
from jax.experimental.pallas import tpu as pltpu
from jax.sharding import PartitionSpec as P

ROPE_THETA = 500000.0
NORM_EPS = 1e-5
LOG2E = 1.4426950408889634
UNROLL = 8


def rope_tables(positions, head_dim):
    inv_freq = ROPE_THETA ** (-jnp.arange(0, head_dim, 2, dtype=jnp.float32) / head_dim)
    angles = positions.astype(jnp.float32)[:, None] * inv_freq[None, :]
    return jnp.cos(angles), jnp.sin(angles)


def apply_rope(values, cos_tab, sin_tab):
    half_dim = values.shape[-1] // 2
    first_half = values[..., :half_dim]
    second_half = values[..., half_dim:]
    cos_rows = cos_tab[:, None, :]
    sin_rows = sin_tab[:, None, :]
    return jnp.concatenate([first_half * cos_rows - second_half * sin_rows, second_half * cos_rows + first_half * sin_rows], axis=-1)


def rms_norm(values, gain_vec):
    vals32 = values.astype(jnp.float32)
    inv_rms = lax.rsqrt(jnp.mean(vals32 * vals32, axis=-1, keepdims=True) + NORM_EPS)
    return (vals32 * inv_rms * gain_vec.astype(jnp.float32)).astype(jnp.bfloat16)


def attn_kernel(cfg, *refs):
    groups, tp, kv_heads, ratio, head_dim, key_rows, rows = (cfg[k] for k in ('groups', 'tp', 'kv_heads', 'ratio', 'head_dim', 'key_rows', 'rows'))
    heads = kv_heads * ratio
    (q_raw, cos_ref, sin_ref, pre_ref, suf_ref, w_ref, o_full, w_full, q_ref, kv_scr, s_scr, o_scr, st_scr, kv_send, kv_recv, o_send, o_recv, o_local,
     wn_send, wn_recv, wf_send, wf_recv, wx_send, wx_recv, ws_send, ws_recv) = refs
    me, my_tp = lax.axis_index('cp'), lax.axis_index('tp')
    my_x, my_core = me // 2, me % 2
    half = key_rows // 2
    scale = (head_dim ** -0.5) * LOG2E
    MESH = pl.DeviceIdType.MESH
    sib = {'cp': my_x * 2 + (1 - my_core)}
    x_next = {'cp': (me + 2) % groups}
    x_prev = {'cp': (me + groups - 2) % groups}
    above, below = {'tp': (my_tp + 1) % tp}, {'tp': (my_tp + tp - 1) % tp}

    barrier = pltpu.get_barrier_semaphore()
    greet = [above, below, sib, x_next, x_prev]
    for dev in greet:
        pl.semaphore_signal(barrier, inc=1, device_id=dev, device_id_type=MESH)
    pl.semaphore_wait(barrier, len(greet))

    def kv_copy(part, g, slot):
        base = part * groups
        src_own = (pre_ref, suf_ref)[part].at[g]
        dst = kv_scr.at[g, base + slot]
        if slot == 0:
            return pltpu.make_async_copy(src_own, dst, kv_recv.at[g, base])
        if slot in (1, 2, 3):
            src = src_own
        elif slot in (4, 5):
            src = kv_scr.at[g, base + slot - 2]
        elif slot == 6:
            src = kv_scr.at[g, base + (2 if g == 0 else 3)]
        else:
            src = kv_scr.at[g, base + 6]
        dev = {1: sib, 4: sib, 5: sib, 7: sib, 2: x_next, 3: x_prev, 6: x_next if g == 0 else x_prev}[slot]
        return pltpu.make_async_remote_copy(src_ref=src, dst_ref=dst, send_sem=kv_send.at[g, base + slot], recv_sem=kv_recv.at[g, base + slot], device_id=dev, device_id_type=MESH)

    gs = range(kv_heads)

    def start(part, slots):
        for slot in slots:
            for g in gs:
                kv_copy(part, g, slot).start()

    def arrived(part, slots):
        for slot in slots:
            for g in gs:
                copy = kv_copy(part, g, slot)
                copy.wait() if slot == 0 else copy.wait_recv()

    n_pre = 2 * groups

    quarter = w_ref.shape[0] // 4
    w_half = quarter // 2
    my_quarter = 2 * (my_x % 2) + my_core
    x_quarter = 2 * (1 - my_x % 2) + my_core
    ks = (tp - 1, 1, 2)

    def w_rows(k, which, lo, n):
        return w_full.at[pl.ds(pl.multiple_of(((my_tp + k) % tp) * w_ref.shape[0] + which * quarter + lo, n), n)]

    def remote(src, dst, send, recv, dev):
        return pltpu.make_async_remote_copy(src_ref=src, dst_ref=dst, send_sem=send, recv_sem=recv, device_id=dev, device_id_type=MESH)

    def w_near():
        src = w_ref.at[pl.ds(pl.multiple_of(my_quarter * quarter, quarter), quarter)]
        return [remote(src, w_rows(0, my_quarter, 0, quarter), wn_send.at[i], wn_recv.at[i], dev) for i, dev in enumerate((above, below))]

    def w_far():
        out = []
        for i, (k, dev) in enumerate(((tp - 1, above), (1, below))):
            piece = w_rows(k, my_quarter, i * w_half, w_half)
            out.append(remote(piece, piece, wf_send.at[i], wf_recv.at[i], dev))
        return out

    def w_x(n):
        out = []
        for i, dev in enumerate((x_next, x_prev)):
            piece = w_rows(ks[n], my_quarter, i * w_half, w_half)
            out.append(remote(piece, piece, wx_send.at[i, n], wx_recv.at[i, n], dev))
        return out

    def w_sib(n, second):
        piece = w_rows(ks[n], x_quarter if second else my_quarter, 0, quarter)
        return remote(piece, piece, ws_send.at[int(second), n], ws_recv.at[int(second), n], sib)

    def rope(h, carry):
        cs = pl.ds(pl.multiple_of(h * head_dim, head_dim), head_dim)
        x = q_raw[:, cs]
        q_ref[:, cs] = (x * cos_ref[...] + pltpu.roll(x, head_dim // 2, 1) * sin_ref[...]).astype(q_ref.dtype)
        return carry

    def locate(j):
        b = j - n_pre
        lower = b < groups
        dev = jnp.where(lower, b, 2 * groups - 1 - b)
        rel = (dev // 2 - my_x + groups // 2) % (groups // 2)
        same = dev % 2 == my_core
        s_slot = jnp.where(rel == 0, jnp.where(same, 0, 1), jnp.where(rel == 1, jnp.where(same, 3, 5), jnp.where(rel == 2, jnp.where(same, 6, 7), jnp.where(same, 2, 4))))
        pre = j < n_pre
        return jnp.where(pre, j // 2, groups + s_slot), jnp.where(pre, (j % 2) * half, jnp.where(lower, 0, half))

    def head_pass(upper, h, lo, hi, suffix, load, store):
        g = h // ratio
        blk = (2 * groups - 1 - me) if upper else me
        q = q_ref[upper * rows:(upper + 1) * rows, pl.ds(pl.multiple_of(h * head_dim, head_dim), head_dim)]

        def scores(j):
            slot, off = locate(j)
            k = kv_scr[g, slot, pl.ds(pl.multiple_of(off, half), half), :]
            return lax.dot_general(k, q, (((1,), (1,)), ((), ())), preferred_element_type=jnp.float32)

        def values_t(j):
            slot, off = locate(j)
            v = kv_scr[g, slot, pl.ds(pl.multiple_of(key_rows + off, half), half), :]
            return jnp.concatenate([v[i * head_dim:(i + 1) * head_dim] for i in range(half // head_dim)], axis=1)

        def update(s, v, state):
            m, l, acc = state
            n = s.shape[0]
            folded = jnp.max(s.reshape(n // 8, 8, rows), axis=0)
            m_new = jnp.maximum(m, jnp.max(folded, axis=0, keepdims=True))
            a = jnp.exp2((m - m_new) * scale)
            p = jnp.exp2(s * scale - m_new * scale)
            l = l * a + jnp.sum(p.reshape(n // 8, 8, rows), axis=0)
            acc = acc * a + jnp.dot(v, p.astype(jnp.bfloat16), preferred_element_type=jnp.float32)
            return m_new, l, acc

        last = n_pre + blk if suffix else hi - 1
        if load:
            i = upper * heads + h
            state = (st_scr[i, head_dim + 8:head_dim + 9], st_scr[i, head_dim:head_dim + 8], st_scr[i, :head_dim])
        else:
            state = (jnp.full((1, rows), -jnp.inf, jnp.float32), jnp.zeros((8, rows), jnp.float32), jnp.zeros((head_dim, rows), jnp.float32))
        s_scr[0] = scores(lo)

        def make_body(base, unroll):
            def body(i, st):
                for u in range(unroll):
                    j = base + i * unroll + u
                    s_scr[(u + 1) % 2] = scores(jnp.minimum(j + 1, last))
                    st = update(s_scr[u % 2], values_t(j), st)
                return st
            return body

        unroll = UNROLL if (hi - lo) % UNROLL == 0 else 4
        state = lax.fori_loop(0, (hi - lo) // unroll, make_body(lo, unroll), state)
        if suffix:
            state = lax.fori_loop(0, blk // 4, make_body(n_pre, 4), state)

            def rest_body(i, st):
                j = last - blk % 4 + i
                s_scr[(i + 1) % 2] = scores(j + 1)
                return update(s_scr[i % 2], values_t(j), st)

            state = lax.fori_loop(0, blk % 4, rest_body, state)
            s = s_scr[blk % 2]
            kid = lax.broadcasted_iota(jnp.int32, s.shape, 0)
            qid = lax.broadcasted_iota(jnp.int32, s.shape, 1)
            state = update(jnp.where(kid <= qid, s, -jnp.inf), values_t(last), state)
        m, l, acc = state
        if store:
            i = upper * heads + h
            st_scr[i, :head_dim] = acc
            st_scr[i, head_dim:head_dim + 8] = l
            st_scr[i, head_dim + 8:] = jnp.broadcast_to(m, (8, rows))
        else:
            o_scr[upper * heads + h] = (acc / jnp.sum(l, axis=0, keepdims=True)).T.astype(o_scr.dtype)

    def o_piece(upper, h, k, lo, n):
        col = ((my_tp + k) % tp) * heads * head_dim + h * head_dim
        return o_full.at[upper * rows + lo:upper * rows + lo + n, pl.ds(pl.multiple_of(col, head_dim), head_dim)]

    def o_near(upper, h):
        i = upper * heads + h
        return [remote(o_scr.at[i], o_piece(upper, h, 0, 0, rows), o_send.at[k, i], o_recv.at[k, i], dev) for k, dev in enumerate((above, below))]

    def o_far(upper, h):
        i = upper * heads + h
        n = rows // 2
        lower_piece, upper_piece = o_piece(upper, h, tp - 1, 0, n), o_piece(upper, h, 1, n, n)
        return [remote(lower_piece, lower_piece, o_send.at[2, i], o_recv.at[2, i], above), remote(upper_piece, upper_piece, o_send.at[3, i], o_recv.at[3, i], below)]

    def o_own(upper, h):
        i = upper * heads + h
        return pltpu.make_async_copy(o_scr.at[i], o_piece(upper, h, 0, 0, rows), o_local.at[i])

    def forward(upper, h):
        for copy in o_near(upper, h):
            copy.wait_recv()
        for copy in o_far(upper, h):
            copy.start()

    def loop_heads(upper, lo_h, hi_h, lo, hi, suffix, load):
        def body(h, carry):
            head_pass(upper, h, lo, hi, suffix, load, not suffix)
            if suffix:
                o_own(upper, h).start()
                for copy in o_near(upper, h):
                    copy.start()

                @pl.when(h > 0)
                def _():
                    forward(upper, h - 1)
            return carry
        lax.fori_loop(lo_h, hi_h, body, 0)

    start(0, (0, 1, 2, 3))
    for copy in w_near():
        copy.start()
    start(1, (0, 1, 2, 3))
    lax.fori_loop(0, heads, rope, 0)
    arrived(0, (0, 1))
    loop_heads(0, 0, heads, 0, 4, False, False)
    arrived(0, (2, 3))
    start(0, (4, 5, 6))
    loop_heads(0, 0, heads, 4, 8, False, True)
    arrived(0, (4, 5))
    loop_heads(0, 0, heads, 8, 12, False, True)
    arrived(0, (6,))
    start(0, (7,))
    arrived(1, (0, 1, 2, 3))
    start(1, (4, 5, 6))
    for copy in w_near():
        copy.wait_recv()
    for copy in w_far():
        copy.start()
    for n in range(2):
        w_sib(n, False).start()
        for copy in w_x(n):
            copy.start()
    loop_heads(1, 0, heads, 0, 8, False, False)
    arrived(0, (7,))
    arrived(1, (4, 5, 6))
    start(1, (7,))
    arrived(1, (7,))
    loop_heads(0, 0, heads, 12, 16, True, True)
    forward(0, heads - 1)
    for copy in w_far():
        copy.wait_recv()
    w_sib(2, False).start()
    for copy in w_x(2):
        copy.start()
    loop_heads(1, 0, heads // 2, 8, 16, True, True)
    for n in range(3):
        for copy in w_x(n):
            copy.wait_recv()
        w_sib(n, True).start()
    loop_heads(1, heads // 2, heads, 8, 16, True, True)
    forward(1, heads - 1)

    for g in gs:
        for part in range(2):
            for slot in range(1, groups):
                kv_copy(part, g, slot).wait_send()
    for copy in w_near() + w_far():
        copy.wait_send()
    for n in range(3):
        for copy in w_x(n):
            copy.wait_send()
        for second in (False, True):
            w_sib(n, second).wait()

    for upper in range(2):
        def drain(h, carry):
            o_own(upper, h).wait()
            for copy in o_near(upper, h):
                copy.wait_send()
            for copy in o_far(upper, h):
                copy.wait()
            return carry
        lax.fori_loop(0, heads, drain, 0)


def attention(q, cos, sin, pre, suf, w_out, cfg):
    groups, tp, kv_heads, ratio, head_dim, key_rows, rows = (cfg[k] for k in ('groups', 'tp', 'kv_heads', 'ratio', 'head_dim', 'key_rows', 'rows'))
    heads = kv_heads * ratio
    bf, f32, dma = jnp.bfloat16, jnp.float32, pltpu.SemaphoreType.DMA
    any_spec = pl.BlockSpec(memory_space=pl.ANY)
    whole = lambda arr: pl.BlockSpec(arr.shape, lambda i: (0, 0))
    kv_shape = (kv_heads, 2 * groups, 2 * key_rows, head_dim)
    kv_sem, o_sem = dma((kv_heads, 2 * groups)), dma((4, 2 * heads))
    scratch = [pltpu.VMEM(q.shape, bf), pltpu.VMEM(kv_shape, bf), pltpu.VMEM((2, key_rows // 2, rows), f32), pltpu.VMEM((2 * heads, rows, head_dim), bf),
               pltpu.VMEM((2 * heads, head_dim + 16, rows), f32), kv_sem, kv_sem, o_sem, o_sem, dma((2 * heads,)),
               dma((2,)), dma((2,)), dma((2,)), dma((2,)), dma((2, 3)), dma((2, 3)), dma((2, 3)), dma((2, 3))]
    n_keys = (4 * groups + 2 * groups) * (key_rows // 2)
    return pl.pallas_call(
        functools.partial(attn_kernel, cfg),
        grid=(1,),
        in_specs=[whole(q), whole(cos), whole(sin)] + [any_spec] * 3,
        out_specs=(any_spec, any_spec),
        out_shape=(jax.ShapeDtypeStruct((2 * rows, tp * heads * head_dim), bf), jax.ShapeDtypeStruct((tp * w_out.shape[0], w_out.shape[1]), bf)),
        scratch_shapes=scratch,
        compiler_params=pltpu.CompilerParams(vmem_limit_bytes=60 * 2**20, dimension_semantics=("arbitrary",), collective_id=0, has_side_effects=True),
        cost_estimate=pl.CostEstimate(flops=rows * heads * n_keys * 4 * head_dim, bytes_accessed=16 * 2**20, transcendentals=rows * heads * n_keys),
        name="attn",
    )(q, cos, sin, pre, suf, w_out)


CHUNK = 256
TILE = 512
N_BUF = 3


def mlp_kernel(cfg, *refs):
    tp, n_o = cfg['tp'], cfg['n_o']
    x_ref = refs[0]
    o_refs = refs[1:1 + n_o]
    (wo_ref, wown_ref, gain_ref, wg_ref, wu_ref, wd_ref, out_ref, wbuf, o_buf, x_buf, y_scr, h_scr, act_scr, part, y_mine, far_buf, near_buf, mine,
     w_sem, in_sem, far_send, far_recv, near_send, near_recv, ag_send, ag_recv, fwd_send, fwd_recv, own_sem) = refs[1 + n_o:]
    rows, width = x_ref.shape
    ff = wg_ref.shape[1]
    n_chunks = rows // CHUNK
    shard = CHUNK // tp
    half = shard // 2
    n_wo, n_gu, n_dn = width // TILE, ff // (TILE // 2), width // TILE
    per = n_wo + n_gu + n_dn
    total = per * n_chunks
    my_tp = lax.axis_index('tp')
    MESH = pl.DeviceIdType.MESH
    above, below = {'tp': (my_tp + 1) % tp}, {'tp': (my_tp + tp - 1) % tp}

    barrier = pltpu.get_barrier_semaphore()
    for dev in (above, below):
        pl.semaphore_signal(barrier, inc=1, device_id=dev, device_id_type=MESH)
    pl.semaphore_wait(barrier, 2)

    def cols(i, n):
        return pl.ds(pl.multiple_of(i * n, n), n)

    def tile_copies(kind, i, slot):
        if kind == 0:
            n = wown_ref.shape[0]
            out = []
            for k in range(tp):
                part_rows = pl.ds(pl.multiple_of(((my_tp + k) % tp) * n, n), n)
                src = wo_ref.at[part_rows, cols(i, TILE)] if k else wown_ref.at[:, cols(i, TILE)]
                out.append(pltpu.make_async_copy(src, wbuf.at[slot, part_rows], w_sem.at[slot, k]))
            return out
        if kind == 1:
            h = TILE // 2
            return [pltpu.make_async_copy(wg_ref.at[:, cols(i, h)], wbuf.at[slot, :, pl.ds(0, h)], w_sem.at[slot, 0]),
                    pltpu.make_async_copy(wu_ref.at[:, cols(i, h)], wbuf.at[slot, :, pl.ds(h, h)], w_sem.at[slot, 1])]
        return [pltpu.make_async_copy(wd_ref.at[:, cols(i, TILE)], wbuf.at[slot, pl.ds(0, ff)], w_sem.at[slot, 0])]

    def fetch(g):
        t = g % per
        slot = g % N_BUF
        for kind, lo, hi in ((0, 0, n_wo), (1, n_wo, n_wo + n_gu), (2, n_wo + n_gu, per)):
            @pl.when((g < total) & (t >= lo) & (t < hi))
            def _():
                for copy in tile_copies(kind, t - lo, slot):
                    copy.start()

    def tile_loop(c, kind, lo, n, use):
        def body(i, carry):
            g = c * per + lo + i
            slot = g % N_BUF
            for copy in tile_copies(kind, i, slot):
                copy.wait()
            fetch(g + N_BUF - 1)
            use(i, slot)
            return carry
        lax.fori_loop(0, n, body, 0)

    def chunk_rows(c):
        return pl.ds(pl.multiple_of(c * CHUNK, CHUNK), CHUNK)

    def input_copies(c, which):
        o_rows = rows // n_o // CHUNK
        return [pltpu.make_async_copy(x_ref.at[chunk_rows(c)], x_buf, in_sem.at[0]),
                pltpu.make_async_copy(o_refs[which].at[chunk_rows(c - which * o_rows)], o_buf, in_sem.at[1])]

    def fetch_inputs(c):
        o_rows = rows // n_o // CHUNK
        for which in range(n_o):
            @pl.when((c < n_chunks) & (c >= which * o_rows) & (c < (which + 1) * o_rows))
            def _():
                for copy in input_copies(c, which):
                    copy.start()

    def owner_rows(k, lo, n):
        return pl.ds(pl.multiple_of(((my_tp + k) % tp) * shard + lo, n), n)

    def remote(src, dst, send, recv, dev):
        return pltpu.make_async_remote_copy(src_ref=src, dst_ref=dst, send_sem=send, recv_sem=recv, device_id=dev, device_id_type=MESH)

    def far_copies(c):
        p = c % 2
        return [remote(part.at[p, owner_rows(2, 0, half)], far_buf.at[c, 0], far_send.at[c, 0], far_recv.at[c, 0], above),
                remote(part.at[p, owner_rows(2, half, half)], far_buf.at[c, 1], far_send.at[c, 1], far_recv.at[c, 1], below)]

    def near_copies(c):
        p = c % 2
        return [remote(part.at[p, owner_rows(1, 0, shard)], near_buf.at[c, 0], near_send.at[c, 0], near_recv.at[c, 0], above),
                remote(part.at[p, owner_rows(tp - 1, 0, shard)], near_buf.at[c, 1], near_send.at[c, 1], near_recv.at[c, 1], below)]

    def out_rows(c, k, lo, n):
        return out_ref.at[pl.ds(pl.multiple_of(c * CHUNK + ((my_tp + k) % tp) * shard + lo, n), n)]

    def gather_copies(c):
        dst = out_rows(c, 0, 0, shard)
        return [remote(mine.at[c], dst, ag_send.at[c, 0], ag_recv.at[c, 0], above),
                remote(mine.at[c], dst, ag_send.at[c, 1], ag_recv.at[c, 1], below)]

    def forward_copies(c):
        lower, upper = out_rows(c, tp - 1, 0, half), out_rows(c, 1, half, half)
        return [remote(lower, lower, fwd_send.at[c, 0], fwd_recv.at[c, 0], above),
                remote(upper, upper, fwd_send.at[c, 1], fwd_recv.at[c, 1], below)]

    def own_copy(c):
        return pltpu.make_async_copy(mine.at[c], out_rows(c, 0, 0, shard), own_sem.at[c])

    def send_far(c):
        for copy in far_copies(c):
            copy.start()

    def send_near(c):
        for copy in far_copies(c):
            copy.wait_recv()
        p = c % 2

        def add(i, carry):
            cs = cols(i, TILE)
            part[p, owner_rows(1, 0, half), cs] += far_buf[c, 0, :, cs]
            part[p, owner_rows(tp - 1, half, half), cs] += far_buf[c, 1, :, cs]
            return carry
        lax.fori_loop(0, width // TILE, add, 0)
        for copy in near_copies(c):
            copy.start()

    def send_result(c):
        for copy in near_copies(c):
            copy.wait_recv()
        p = c % 2

        def add(i, carry):
            cs = cols(i, TILE)
            total_rows = part[p, owner_rows(0, 0, shard), cs] + near_buf[c, 0, :, cs] + near_buf[c, 1, :, cs]
            mine[c, :, cs] = (y_mine[p, :, cs] + total_rows).astype(mine.dtype)
            return carry
        lax.fori_loop(0, width // TILE, add, 0)
        own_copy(c).start()
        for copy in gather_copies(c):
            copy.start()
        for copy in far_copies(c) + near_copies(c):
            copy.wait_send()

    def forward_result(c):
        for copy in gather_copies(c):
            copy.wait_recv()
        for copy in forward_copies(c):
            copy.start()

    fetch_inputs(0)
    for g in range(N_BUF - 1):
        fetch(g)

    def chunk_body(c, carry):
        p = c % 2
        for copy in input_copies(0, 0):
            copy.wait()

        def proj(i, slot):
            cs = cols(i, TILE)
            y_scr[:, cs] = x_buf[:, cs].astype(jnp.float32) + jnp.dot(o_buf[...], wbuf[slot], preferred_element_type=jnp.float32)

        tile_loop(c, 0, 0, n_wo, proj)
        fetch_inputs(c + 1)

        def square(i, acc):
            y = y_scr[:, cols(i, TILE)]
            y2 = y * y
            for k in range(TILE // 128):
                acc = acc + y2[:, k * 128:(k + 1) * 128]
            return acc
        acc = lax.fori_loop(0, width // TILE, square, jnp.zeros((CHUNK, 128), jnp.float32))
        inv_rms = lax.rsqrt(jnp.sum(acc, axis=1, keepdims=True) / width + NORM_EPS)

        def norm(i, carry):
            cs = cols(i, TILE)
            h_scr[:, cs] = (y_scr[:, cs] * inv_rms * gain_ref[:, cs].astype(jnp.float32)).astype(h_scr.dtype)
            y_mine[p, :, cs] = y_scr[owner_rows(0, 0, shard), cs]
            return carry
        lax.fori_loop(0, width // TILE, norm, 0)

        @pl.when(c > 0)
        def _():
            send_near(c - 1)

        @pl.when(c > 1)
        def _():
            forward_result(c - 2)

        def gated(i, slot):
            gu = jnp.dot(h_scr[...], wbuf[slot], preferred_element_type=jnp.float32)
            gate, up = gu[:, :TILE // 2], gu[:, TILE // 2:]
            act_scr[:, cols(i, TILE // 2)] = (gate * lax.logistic(gate) * up).astype(act_scr.dtype)

        tile_loop(c, 1, n_wo, n_gu, gated)

        @pl.when(c > 0)
        def _():
            send_result(c - 1)

        def down(i, slot):
            part[p, :, cols(i, TILE)] = jnp.dot(act_scr[...], wbuf[slot, :ff], preferred_element_type=jnp.float32)

        tile_loop(c, 2, n_wo + n_gu, n_dn, down)
        send_far(c)
        return carry

    lax.fori_loop(0, n_chunks, chunk_body, 0)
    send_near(n_chunks - 1)
    forward_result(n_chunks - 2)
    send_result(n_chunks - 1)
    forward_result(n_chunks - 1)

    def drain(c, carry):
        own_copy(c).wait()
        for copy in gather_copies(c):
            copy.wait_send()
        for copy in forward_copies(c):
            copy.wait()
        return carry
    lax.fori_loop(0, n_chunks, drain, 0)


def mlp_block(x, o_parts, w_out, w_own, gain, w_gate, w_up, w_down, tp):
    rows, width = x.shape
    ff = w_gate.shape[1]
    n = rows // CHUNK
    shard = CHUNK // tp
    any_spec = pl.BlockSpec(memory_space=pl.ANY)
    bf, f32, dma = jnp.bfloat16, jnp.float32, pltpu.SemaphoreType.DMA
    pair = dma((n, 2))
    scratch = [pltpu.VMEM((N_BUF, width, TILE), bf), pltpu.VMEM((CHUNK, width), bf), pltpu.VMEM((CHUNK, width), bf), pltpu.VMEM((CHUNK, width), f32),
               pltpu.VMEM((CHUNK, width), bf), pltpu.VMEM((CHUNK, ff), bf), pltpu.VMEM((2, CHUNK, width), f32), pltpu.VMEM((2, shard, width), f32),
               pltpu.VMEM((n, 2, shard // 2, width), f32), pltpu.VMEM((n, 2, shard, width), f32), pltpu.VMEM((n, shard, width), bf),
               dma((N_BUF, tp)), dma((2,)), pair, pair, pair, pair, pair, pair, pair, pair, dma((n,))]
    flops = 2 * rows * width * (w_out.shape[0] + 3 * ff)
    return pl.pallas_call(
        functools.partial(mlp_kernel, dict(tp=tp, n_o=len(o_parts))),
        grid=(1,),
        in_specs=[any_spec] * (3 + len(o_parts)) + [pl.BlockSpec((1, width), lambda i: (0, 0))] + [any_spec] * 3,
        out_specs=any_spec,
        out_shape=jax.ShapeDtypeStruct(x.shape, x.dtype),
        scratch_shapes=scratch,
        compiler_params=pltpu.CompilerParams(vmem_limit_bytes=63 * 2**20, dimension_semantics=("arbitrary",), collective_id=2, has_side_effects=True),
        cost_estimate=pl.CostEstimate(flops=flops, bytes_accessed=500 * 2**20, transcendentals=rows * ff),
        name="mlp",
    )(x, *o_parts, w_out, w_own, gain.reshape(1, width), w_gate, w_up, w_down)


def solution(mesh):
    groups = mesh.shape['cp']
    tp = mesh.shape['tp']

    def local_layer(x_loc, kp_loc, vp_loc, norm_attn, w_query, w_key, w_value, w_out, norm_mlp, w_gate, w_up, w_down):
        rows_loc = x_loc.shape[0]
        blk_len = rows_loc // 2
        pre_dev, kv_loc, head_dim = kp_loc.shape
        heads_loc = w_query.shape[1] // head_dim
        prefix_len = pre_dev * groups
        my_cp = lax.axis_index('cp')

        def bundle_of(k, v):
            kt = jnp.moveaxis(k, 1, 0)
            vt = v.reshape(rows_loc // head_dim, head_dim, kv_loc, head_dim).transpose(2, 0, 3, 1).reshape(kv_loc, rows_loc, head_dim)
            return jnp.concatenate([kt, vt], axis=1)

        local_row = jnp.arange(rows_loc, dtype=jnp.int32)
        blk_idx = jnp.where(local_row < blk_len, my_cp, 2 * groups - 1 - my_cp)
        q_pos = prefix_len + blk_idx * blk_len + local_row % blk_len
        cos_tab, sin_tab = rope_tables(q_pos, head_dim)
        hidden = rms_norm(x_loc, norm_attn)
        k_proj = jnp.dot(hidden, w_key, preferred_element_type=jnp.float32).reshape(rows_loc, kv_loc, head_dim)
        k_new = apply_rope(k_proj, cos_tab, sin_tab).astype(jnp.bfloat16)
        v_new = jnp.dot(hidden, w_value, preferred_element_type=jnp.float32).astype(jnp.bfloat16).reshape(rows_loc, kv_loc, head_dim)
        q_proj = jnp.dot(hidden, w_query, preferred_element_type=jnp.float32)
        cos_all = jnp.concatenate([cos_tab, cos_tab], axis=1)
        sin_all = jnp.concatenate([-sin_tab, sin_tab], axis=1)

        cfg = dict(groups=groups, tp=tp, kv_heads=kv_loc, ratio=heads_loc // kv_loc, head_dim=head_dim, key_rows=rows_loc, rows=blk_len)
        o_full, w_full = attention(q_proj, cos_all, sin_all, bundle_of(kp_loc, vp_loc), bundle_of(k_new, v_new), w_out, cfg)
        x_out = mlp_block(x_loc, [o_full], w_full, w_out, norm_mlp, w_gate, w_up, w_down, tp)
        return x_out, k_new, v_new

    row_spec = P(('dp', 'cp'), None)
    kv_spec = P(('dp', 'cp'), 'tp', None)
    col_spec = P(None, 'tp')
    row_split = P('tp', None)
    vec_spec = P(None)
    return jax.shard_map(local_layer, mesh=mesh, in_specs=(row_spec, kv_spec, kv_spec, vec_spec, col_spec, col_spec, col_spec, row_split, vec_spec, col_spec, col_spec, row_split), out_specs=(row_spec, kv_spec, kv_spec), check_vma=False)
```
